32 devices in a mesh: groups: 2 (over x), seq: 4 (over y, core), head: 4 (over z).
Axes of the slice: x: 2, y: 2, z: 4, core: 2. Of those that a mesh axis runs over, the one named last changes fastest.
Arguments:
- query: bfloat16 [32, 16, 1024], P('groups', None, 'head'), parts along dimension 0, may hold values from -6 to 6, as said below
- new_key: bfloat16 [32, 16, 1024], P('groups', None, 'head'), parts along dimension 0, may hold values from -6 to 6
- new_value: bfloat16 [32, 16, 1024], P('groups', None, 'head'), parts along dimension 0, may hold values from -6 to 6
- keys: bfloat16 [32, 4096, 1024], P('groups', 'seq', 'head'), parts along dimension 0, may hold values from -6 to 6, as said below
- values: bfloat16 [32, 4096, 1024], P('groups', 'seq', 'head'), parts along dimension 0, may hold values from -6 to 6
- lengths: int32 [32], P('groups'), parts along dimension 0, may hold values from 2 to 4096
- time_bucket: int32 [32, 4096], P('groups', 'seq'), parts along dimension 0, may hold values from 0 to 63
- action: int32 [32, 4096], P('groups', 'seq'), parts along dimension 0, may hold values from 0 to 15
- time_bias: float32 [64, 8], P(None, 'head'), may hold values from -0.25 to 0.25
- action_bias: float32 [16, 8], P(None, 'head'), may hold values from -0.25 to 0.25
- gate: bfloat16 [32, 16, 1024], P('groups', None, 'head'), parts along dimension 0, may hold values from -6 to 6
- norm_gain: float32 [1024], P('head'), may hold values from 0.1 to 1.9
- w_out: bfloat16 [1024, 1024], P('head'), may hold values from -0.1875 to 0.1875
Outputs:
- output: bfloat16 [32, 16, 1024], P(('groups', 'seq'), None, 'head'), parts along dimension 0
The draws below stay inside these ranges and needn't reach their ends.
There are 2 independent parts, one for each index of `groups`. The reference program is written for one: setup_inputs(seed, part) draws one part's arguments, and reference() takes and returns one part's arrays. A program takes and returns all parts, laid end to end along the dimension named above; an argument that names none is the same for every part. Nothing has to cross between parts.
Inputs may be any that keep to these rules, and one draw needn't show every extreme that they name: `query`: queries of order one; some users' queries may be large and equal to some of their keys. `keys`: keys of order one.
All inputs are finite; a program needn't handle non-finite values.
Results may differ from the reference program's by a relative error of at most 0.0056.
Values sent between devices are 32-bit elements; how exact they have to be, the bound alone decides.
A program may use at most 64 MiB of HBM per device.

```python
import math
import jax
import jax.numpy as jnp
from jax import lax

USERS = 16
CANDS = 16
S_DEV = 1024
HEADS = 8
DH = 128
D_MODEL = 1024
BUCKETS = 64
ACTIONS = 16
HISTORY = 4096
N_SEQ = 4


def draw_query(key, part):
    result = jax.random.truncated_normal(jax.random.fold_in(key, 1), -6.0, 6.0, (USERS, CANDS, HEADS * DH), jnp.float32)
    return result.astype(jnp.bfloat16)


def draw_keys(key, part):
    result = jax.random.truncated_normal(jax.random.fold_in(key, 2), -6.0, 6.0, (USERS, HISTORY, HEADS * DH), jnp.float32)
    return result.astype(jnp.bfloat16)


def plant(values, key, smallest, top_value):
    place = [jax.random.randint(jax.random.fold_in(key, axis), (), 0, length) for axis, length in enumerate(values.shape)]
    widest = values.shape.index(max(values.shape))
    beside = place[:widest] + [(place[widest] + 1) % values.shape[widest]] + place[widest + 1:]
    return values.at[tuple(place)].set(smallest).at[tuple(beside)].set(top_value)


def block_levels(key, dims, split, least, largest):
    def one(dim, blocks):
        steps = jax.random.uniform(jax.random.fold_in(jax.random.fold_in(key, 6), dim), (blocks,), jnp.float32, least / len(split), largest / len(split))
        return jnp.repeat(jnp.exp(steps), dims[dim] // blocks).reshape((-1,) + (1,) * (len(dims) - dim - 1))

    gain = one(*split[0])
    for cut in split[1:]:
        gain = gain * one(*cut)
    return gain


def noise(stream_key, extent, scale, bound, split=(), held_as=jnp.bfloat16):
    values = scale * jax.random.normal(stream_key, extent, jnp.float32)
    if split:
        values = values * block_levels(stream_key, extent, split, -0.22, 0.18)
    return jnp.clip(values, -bound, bound).astype(held_as)


def setup_inputs(seed: int = 0, part: int = 0) -> dict:
    splits = jax.random.split(jax.random.key(seed), 14)
    own_keys = jax.random.split(jax.random.fold_in(splits[13], part), 14)
    return {
        "query": draw_query(jax.random.fold_in(jax.random.fold_in(splits[13], part), 71), part),
        "new_key": noise(own_keys[1], (USERS, CANDS, HEADS * DH), 1.0, 6.0, ((2, 4),)),
        "new_value": noise(own_keys[2], (USERS, CANDS, HEADS * DH), 1.0, 6.0, ((2, 4),)),
        "keys": draw_keys(jax.random.fold_in(jax.random.fold_in(splits[13], part), 71), part),
        "values": noise(own_keys[4], (USERS, HISTORY, HEADS * DH), 1.0, 6.0, ((1, 4), (2, 4))),
        "lengths": plant(jax.random.randint(own_keys[5], (USERS,), 2, HISTORY + 1), jax.random.fold_in(own_keys[5], 1), 2, HISTORY).astype(jnp.int32),
        "time_bucket": plant(jax.random.randint(own_keys[6], (USERS, HISTORY), 0, BUCKETS), jax.random.fold_in(own_keys[6], 1), 0, BUCKETS - 1).astype(jnp.int32),
        "action": plant(jax.random.randint(own_keys[7], (USERS, HISTORY), 0, ACTIONS), jax.random.fold_in(own_keys[7], 1), 0, ACTIONS - 1).astype(jnp.int32),
        "time_bias": jnp.clip(jax.random.uniform(splits[8], (BUCKETS, HEADS), jnp.float32, -0.25, 0.25) * block_levels(splits[8], (BUCKETS, HEADS), ((1, 4),), -0.4, 0.0), -0.25, 0.25),
        "action_bias": jnp.clip(jax.random.uniform(splits[9], (ACTIONS, HEADS), jnp.float32, -0.25, 0.25) * block_levels(splits[9], (ACTIONS, HEADS), ((1, 4),), -0.4, 0.0), -0.25, 0.25),
        "gate": noise(own_keys[10], (USERS, CANDS, HEADS * DH), 1.0, 6.0, ((2, 4),)),
        "norm_gain": jnp.clip(1.0 + 0.18 * jax.random.normal(splits[11], (HEADS * DH,), jnp.float32), 0.1, 1.9),
        "w_out": noise(splits[12], (HEADS * DH, D_MODEL), (HEADS * DH) ** -0.5, 0.1875, ((0, 4),)),
    }


def reference(query, new_key, new_value, keys, values, lengths, time_bucket, action, time_bias, action_bias, gate, norm_gain, w_out):
    user_count = keys.shape[0]
    cand_count = query.shape[1]
    head_count = HEADS
    head_size = DH
    score_scale = 1.0 / math.sqrt(head_size)
    query_heads = query.astype(jnp.float32).reshape(user_count, cand_count, head_count, head_size)

    def one_block(block_index):
        first = (block_index * S_DEV).astype(jnp.int32)
        key_block = lax.dynamic_slice_in_dim(keys, first, S_DEV, 1).astype(jnp.float32).reshape(user_count, S_DEV, head_count, head_size)
        value_block = lax.dynamic_slice_in_dim(values, first, S_DEV, 1).astype(jnp.float32).reshape(user_count, S_DEV, head_count, head_size)
        bucket_block = lax.dynamic_slice_in_dim(time_bucket, first, S_DEV, 1)
        action_block = lax.dynamic_slice_in_dim(action, first, S_DEV, 1)
        scores = jnp.einsum('uchd,ushd->uchs', query_heads, key_block) * score_scale
        biases = jnp.transpose(time_bias[bucket_block], (0, 2, 1)) + jnp.transpose(action_bias[action_block], (0, 2, 1))
        scores = scores + biases[:, None]
        position = first + jnp.arange(S_DEV, dtype=jnp.int32)
        valid = position[None, None, None, :] < lengths[:, None, None, None]
        block_max = lax.optimization_barrier(jnp.max(jnp.where(valid, scores, -1e+30), axis=-1))
        weights = jnp.where(valid, jnp.exp(scores - block_max[..., None]), 0.0)
        block_sum = lax.optimization_barrier(jnp.sum(weights, axis=-1))
        rounded = weights.astype(jnp.bfloat16).astype(jnp.float32)
        block_acc = jnp.einsum('uchs,ushd->uchd', rounded, value_block)
        return (block_max, block_sum, block_acc)
    maxima, sums, accs = lax.map(one_block, jnp.arange(N_SEQ, dtype=jnp.int32))
    own = lax.optimization_barrier(jnp.sum(query_heads * new_key.astype(jnp.float32).reshape(user_count, cand_count, head_count, head_size), axis=-1)) * score_scale
    overall = jnp.maximum(lax.optimization_barrier(jnp.max(maxima, axis=0)), own)
    factors = jnp.exp(maxima - overall[None])
    own_factor = jnp.exp(own - overall)
    numer = lax.optimization_barrier(jnp.sum(factors[..., None] * accs, axis=0)) + own_factor[..., None] * new_value.astype(jnp.float32).reshape(user_count, cand_count, head_count, head_size)
    denom = lax.optimization_barrier(jnp.sum(factors * sums, axis=0)) + own_factor
    attended = numer / denom[..., None]
    square_sum = lax.optimization_barrier(jnp.sum(jnp.square(attended), axis=(2, 3)))
    gate_heads = gate.astype(jnp.float32).reshape(user_count, cand_count, head_count, head_size)
    hidden = (attended * norm_gain.reshape(head_count, head_size) * jax.nn.silu(gate_heads)).astype(jnp.bfloat16)
    hidden = hidden.reshape(user_count * cand_count, head_count * head_size)
    projected = jnp.dot(hidden, w_out, preferred_element_type=jnp.float32).reshape(user_count, cand_count, -1)
    factor = 1.0 / jnp.sqrt(square_sum / (head_count * head_size) + 1e-06)
    return (projected * factor[:, :, None]).astype(jnp.bfloat16)
```

```python
import functools
import math

import jax
import jax.numpy as jnp
from jax import lax
from jax.experimental import pallas as pl
from jax.experimental.pallas import tpu as pltpu
from jax.sharding import PartitionSpec as P

MESH = pl.DeviceIdType.MESH
LANES = 128
LOG2E = math.log2(math.e)
GROUP = 2
LAG = 2
INVALID = -1e30
FLOOR = -1e29
NT = (((1,), (1,)), ((), ()))


def partner(rank, step, count):
    result, bit = 0, 1
    while bit < count:
        held = (rank // bit) % 2
        result = result + bit * (1 - held if (step // bit) % 2 else held)
        bit *= 2
    return result


def column_to_row(column, first, lanes):
    shape = (column.shape[0], lanes)
    row_id = lax.broadcasted_iota(jnp.int32, shape, 0)
    lane_id = lax.broadcasted_iota(jnp.int32, shape, 1)
    return jnp.sum(jnp.where(lane_id == row_id + first, column, 0.0), axis=0, keepdims=True)


def row_to_column(row, first, count):
    shape = (count, row.shape[1])
    row_id = lax.broadcasted_iota(jnp.int32, shape, 0)
    lane_id = lax.broadcasted_iota(jnp.int32, shape, 1)
    return jnp.sum(jnp.where(lane_id == row_id + first, row, 0.0), axis=1, keepdims=True)


def kernel(
    dims,
    len_hbm,
    q_hbm,
    nk_hbm,
    nv_hbm,
    k_hbm,
    v_hbm,
    bucket_hbm,
    action_hbm,
    tb_hbm,
    ab_hbm,
    gate_hbm,
    gain_hbm,
    w_hbm,
    out_ref,
    len_ref,
    q_s,
    nk_s,
    nv_s,
    k_s,
    v_s,
    bucket_s,
    action_s,
    tb_s,
    ab_s,
    gate_s,
    gain_s,
    w_s,
    qd_s,
    bias_s,
    part_s,
    got_s,
    zpart_s,
    zgot_s,
    k_sem,
    v_sem,
    in_sem,
    late_sem,
    send_sem,
    recv_sem,
    zsend_sem,
    zrecv_sem,
):
    users, cands, block, heads, size, seqs, slices, local, out_cols = dims
    rows = heads * cands
    width = heads * size
    me = lax.axis_index("seq")
    mh = lax.axis_index("head")
    scale = LOG2E / math.sqrt(size)

    barrier = pltpu.get_barrier_semaphore()
    for step in range(1, seqs):
        pl.semaphore_signal(
            barrier, inc=1, device_id={"seq": partner(me, step, seqs)}, device_id_type=MESH
        )
    for step in range(1, slices):
        pl.semaphore_signal(
            barrier, inc=1, device_id={"head": (mh + step) % slices}, device_id_type=MESH
        )

    early = [
        pltpu.make_async_copy(source, target, in_sem.at[i])
        for i, (source, target) in enumerate(
            (
                (len_hbm, len_ref),
                (tb_hbm, tb_s),
                (ab_hbm, ab_s),
                (bucket_hbm, bucket_s),
                (action_hbm, action_s),
                (q_hbm, q_s),
            )
        )
    ]
    mine = pl.ds(me * local, local)
    late = [
        pltpu.make_async_copy(source, target, late_sem.at[i])
        for i, (source, target) in enumerate(
            (
                (nk_hbm.at[mine], nk_s),
                (nv_hbm.at[mine], nv_s),
                (gate_hbm.at[mine], gate_s),
                (gain_hbm, gain_s),
                (w_hbm, w_s),
            )
        )
    ]
    for copy in early:
        copy.start()
    order = []
    for turn in range(local):
        for step in range(seqs - 1, -1, -1):
            slot = len(order)
            user = partner(me, step, seqs) * local + turn
            k_copy = pltpu.make_async_copy(k_hbm.at[user], k_s.at[slot], k_sem.at[slot])
            v_copy = pltpu.make_async_copy(v_hbm.at[user], v_s.at[slot], v_sem.at[slot])
            order.append((turn, step, user, k_copy, v_copy))
    for _, _, _, k_copy, v_copy in order:
        k_copy.start(priority=1)
        v_copy.start(priority=1)
    for copy in late:
        copy.start()
    for copy in early:
        copy.wait()

    lane_of = lax.broadcasted_iota(jnp.int32, (users, cands, width), 2)
    query = q_s[...]
    for head in range(heads):
        qd_s[:, head * cands : (head + 1) * cands, :] = jnp.where(
            lane_of // size == head, query, jnp.zeros_like(query)
        )

    def table(ref, head):
        row = ref[head : head + 1, :] * LOG2E
        return jnp.concatenate([row, jnp.zeros((1, LANES - row.shape[1]), row.dtype)], axis=1)

    user_id = lax.broadcasted_iota(jnp.int32, (users, LANES), 0)
    limit = jnp.zeros((users, LANES), jnp.int32)
    for user in range(users):
        limit = jnp.where(user_id == user, len_ref[user], limit)
    limit = limit - me * block - lax.broadcasted_iota(jnp.int32, (users, LANES), 1)
    for head in range(heads):
        tb_row = jnp.broadcast_to(table(tb_s, head), (users, LANES))
        ab_row = jnp.broadcast_to(table(ab_s, head), (users, LANES))
        for chunk in range(block // LANES):
            lanes = slice(chunk * LANES, (chunk + 1) * LANES)
            bias = jnp.take_along_axis(tb_row, bucket_s[:, lanes], axis=1) + jnp.take_along_axis(
                ab_row, action_s[:, lanes], axis=1
            )
            bias_s[head, :, lanes] = jnp.where(limit > chunk * LANES, bias, INVALID)

    def score(slot):
        turn, step, user, _, _ = order[slot]
        raw = lax.dot_general(qd_s[user], k_s[slot], NT, preferred_element_type=jnp.float32)
        bias = jnp.concatenate(
            [
                jnp.broadcast_to(bias_s[head, pl.ds(user, 1), :], (cands, block))
                for head in range(heads)
            ],
            axis=0,
        )
        scores = raw * scale + bias
        top = jnp.maximum(jnp.max(scores, axis=1, keepdims=True), FLOOR)
        weights = jnp.exp2(scores - top)
        total = jnp.sum(weights, axis=1, keepdims=True)
        stats = column_to_row(top, 0, size) + column_to_row(total, rows, size)
        part_s[turn, step, rows : rows + 1, :] = stats
        return weights.astype(jnp.bfloat16)

    def mix(slot, weights):
        turn, step, _, _, _ = order[slot]
        mixed = jnp.dot(weights, v_s[slot], preferred_element_type=jnp.float32)
        for head in range(heads):
            held = slice(head * cands, (head + 1) * cands)
            part_s[turn, step, held, :] = mixed[held, head * size : (head + 1) * size]

    def attend(slots):
        waiting = []
        for slot in slots:
            waiting.append((slot, score(slot)))
            if len(waiting) > 1:
                mix(*waiting.pop(0))
        for item in waiting:
            mix(*item)

    def exchange(turn, step):
        return pltpu.make_async_remote_copy(
            src_ref=part_s.at[turn, step],
            dst_ref=got_s.at[turn, step - 1],
            send_sem=send_sem.at[turn, step - 1],
            recv_sem=recv_sem.at[turn, step - 1],
            device_id={"seq": partner(me, step, seqs)},
            device_id_type=MESH,
        )

    def spread(turn, step):
        target = (mh + step) % slices
        return pltpu.make_async_remote_copy(
            src_ref=zpart_s.at[turn, target],
            dst_ref=zgot_s.at[turn, step - 1],
            send_sem=zsend_sem.at[turn, step - 1],
            recv_sem=zrecv_sem.at[turn, step - 1],
            device_id={"head": target},
            device_id_type=MESH,
        )

    def by_head(source):
        return jnp.concatenate(
            [source[:, head * size : (head + 1) * size] for head in range(heads)], axis=0
        )

    def combine(turn):
        query = q_s[me * local + turn].astype(jnp.float32)
        new_key = nk_s[turn].astype(jnp.float32)
        new_value = nv_s[turn].astype(jnp.float32)
        own = jnp.sum(by_head(query * new_key), axis=1, keepdims=True) * scale
        gate = gate_s[turn].astype(jnp.float32)
        gain = gain_s[...].reshape(1, width)
        gated = gain * (gate / (1.0 + jnp.exp(-gate)))
        for step in range(1, seqs):
            exchange(turn, step).wait_recv()
        blocks = [part_s.at[turn, 0]] + [got_s.at[turn, step - 1] for step in range(1, seqs)]
        maxima = [row_to_column(ref[rows : rows + 1, :], 0, rows) for ref in blocks]
        sums = [row_to_column(ref[rows : rows + 1, :], rows, rows) for ref in blocks]
        top = functools.reduce(jnp.maximum, maxima, own)
        own_factor = jnp.exp2(own - top)
        numer = own_factor * by_head(new_value)
        denom = own_factor
        for ref, high, amount in zip(blocks, maxima, sums):
            factor = jnp.exp2(high - top)
            numer = numer + factor * ref[:rows, :]
            denom = denom + factor * amount
        attended = numer / denom
        squares = jnp.sum(jnp.square(attended), axis=1, keepdims=True)
        square = squares[:cands]
        for head in range(1, heads):
            square = square + squares[head * cands : (head + 1) * cands]
        wide = jnp.concatenate(
            [attended[head * cands : (head + 1) * cands] for head in range(heads)], axis=1
        )
        hidden = (wide * gated).astype(jnp.bfloat16)
        projected = jnp.dot(hidden, w_s[...], preferred_element_type=jnp.float32)
        square_row = column_to_row(square, 0, out_cols)
        for target in range(slices):
            zpart_s[turn, target, :cands, :] = projected[
                :, target * out_cols : (target + 1) * out_cols
            ]
            zpart_s[turn, target, cands : cands + 1, :] = square_row
        for step in range(slices - 1, 0, -1):
            spread(turn, step).start()

    def finish(turn):
        total = zpart_s[turn, mh]
        for step in range(1, slices):
            spread(turn, step).wait_recv()
            total = total + zgot_s[turn, step - 1]
        column = row_to_column(total[cands : cands + 1, :], 0, cands)
        factor = 1.0 / jnp.sqrt(column / (width * slices) + 1e-6)
        out_ref[turn] = (total[:cands] * factor).astype(out_ref.dtype)

    groups = [
        list(range(first, min(first + GROUP, len(order)))) for first in range(0, len(order), GROUP)
    ]
    done = 0
    for index, slots in enumerate(groups):
        for slot in slots:
            order[slot][3].wait()
            order[slot][4].wait()
        attend(slots)
        if index == 0:
            pl.semaphore_wait(barrier, seqs - 1 + slices - 1)
        for slot in slots:
            if order[slot][1]:
                exchange(order[slot][0], order[slot][1]).start()
        if index == 0:
            for copy in late:
                copy.wait()
        while done < local and (done + 1) * seqs + LAG * GROUP <= slots[-1] + 1:
            combine(done)
            done += 1
    while done < local:
        combine(done)
        done += 1
    for turn in range(local):
        finish(turn)
    for turn in range(local):
        for step in range(1, seqs):
            exchange(turn, step).wait_send()
        for step in range(1, slices):
            spread(turn, step).wait_send()


def body(
    query,
    new_key,
    new_value,
    keys,
    values,
    lengths,
    time_bucket,
    action,
    time_bias,
    action_bias,
    gate,
    norm_gain,
    w_out,
):
    users, block, width = keys.shape
    cands = query.shape[1]
    heads = time_bias.shape[1]
    size = width // heads
    seqs = lax.axis_size("seq")
    slices = lax.axis_size("head")
    local = users // seqs
    rows = heads * cands
    out_cols = w_out.shape[1] // slices
    dims = (users, cands, block, heads, size, seqs, slices, local, out_cols)
    f32, bf16 = jnp.float32, jnp.bfloat16
    anywhere = pl.BlockSpec(memory_space=pltpu.HBM)
    return pl.pallas_call(
        functools.partial(kernel, dims),
        out_shape=jax.ShapeDtypeStruct((local, cands, out_cols), bf16),
        in_specs=[anywhere] * 13,
        out_specs=pl.BlockSpec(memory_space=pltpu.VMEM),
        scratch_shapes=[
            pltpu.SMEM((users,), jnp.int32),
            pltpu.VMEM((users, cands, width), bf16),
            pltpu.VMEM((local, cands, width), bf16),
            pltpu.VMEM((local, cands, width), bf16),
            pltpu.VMEM((users, block, width), bf16),
            pltpu.VMEM((users, block, width), bf16),
            pltpu.VMEM((users, block), jnp.int32),
            pltpu.VMEM((users, block), jnp.int32),
            pltpu.VMEM(time_bias.T.shape, f32),
            pltpu.VMEM(action_bias.T.shape, f32),
            pltpu.VMEM((local, cands, width), bf16),
            pltpu.VMEM((width,), f32),
            pltpu.VMEM(w_out.shape, bf16),
            pltpu.VMEM((users, rows, width), bf16),
            pltpu.VMEM((heads, users, block), f32),
            pltpu.VMEM((local, seqs, rows + 1, size), f32),
            pltpu.VMEM((local, seqs - 1, rows + 1, size), f32),
            pltpu.VMEM((local, slices, cands + 1, out_cols), f32),
            pltpu.VMEM((local, slices - 1, cands + 1, out_cols), f32),
            pltpu.SemaphoreType.DMA((users,)),
            pltpu.SemaphoreType.DMA((users,)),
            pltpu.SemaphoreType.DMA((6,)),
            pltpu.SemaphoreType.DMA((5,)),
            pltpu.SemaphoreType.DMA((local, seqs - 1)),
            pltpu.SemaphoreType.DMA((local, seqs - 1)),
            pltpu.SemaphoreType.DMA((local, slices - 1)),
            pltpu.SemaphoreType.DMA((local, slices - 1)),
        ],
        compiler_params=pltpu.CompilerParams(
            collective_id=0, has_side_effects=True, vmem_limit_bytes=52428800
        ),
    )(
        *(
            pltpu.with_memory_space_constraint(x, pltpu.HBM)
            for x in (
                lengths,
                query,
                new_key,
                new_value,
                keys,
                values,
                time_bucket,
                action,
                time_bias.T,
                action_bias.T,
                gate,
                norm_gain,
                w_out,
            )
        )
    )


def solution(mesh):
    placed = (
        P("groups", None, "head"),
        P("groups", None, "head"),
        P("groups", None, "head"),
        P("groups", "seq", "head"),
        P("groups", "seq", "head"),
        P("groups"),
        P("groups", "seq"),
        P("groups", "seq"),
        P(None, "head"),
        P(None, "head"),
        P("groups", None, "head"),
        P("head"),
        P("head", None),
    )
    return jax.shard_map(
        body,
        mesh=mesh,
        in_specs=placed,
        out_specs=P(("groups", "seq"), None, "head"),
        check_vma=False,
    )
```

```python
import functools
import math

import jax
import jax.numpy as jnp
from jax import lax
from jax.experimental import pallas as pl
from jax.experimental.pallas import tpu as pltpu
from jax.sharding import PartitionSpec as P

MESH = pl.DeviceIdType.MESH
LANES = 128
LOG2E = math.log2(math.e)
GROUP = 4
START = 13
INVALID = -1e30
FLOOR = -1e29
NT = (((1,), (1,)), ((), ()))


def partner(rank, step, count):
    result, bit = 0, 1
    while bit < count:
        held = (rank // bit) % 2
        result = result + bit * (1 - held if (step // bit) % 2 else held)
        bit *= 2
    return result


def plan(seqs, local):
    away = list(range(seqs - 1, 0, -1))
    groups = []
    for turn in range(local):
        steps = away + [0] if turn == 0 else away
        for first in range(0, len(steps), GROUP):
            groups.append([(turn, step) for step in steps[first : first + GROUP]])
    groups.extend([(turn, 0)] for turn in range(1, local))
    return groups


def column_to_row(column, first, lanes):
    shape = (column.shape[0], lanes)
    row_id = lax.broadcasted_iota(jnp.int32, shape, 0)
    lane_id = lax.broadcasted_iota(jnp.int32, shape, 1)
    return jnp.sum(jnp.where(lane_id == row_id + first, column, 0.0), axis=0, keepdims=True)


def row_to_column(row, first, count):
    shape = (count, row.shape[1])
    row_id = lax.broadcasted_iota(jnp.int32, shape, 0)
    lane_id = lax.broadcasted_iota(jnp.int32, shape, 1)
    return jnp.sum(jnp.where(lane_id == row_id + first, row, 0.0), axis=1, keepdims=True)


def kernel(
    dims,
    len_hbm,
    q_hbm,
    nk_hbm,
    nv_hbm,
    k_hbm,
    v_hbm,
    bucket_hbm,
    action_hbm,
    tb_hbm,
    ab_hbm,
    gate_hbm,
    gain_hbm,
    w_hbm,
    out_ref,
    len_ref,
    q_s,
    mine_s,
    kv_s,
    event_s,
    tb_s,
    ab_s,
    gain_s,
    w_s,
    qd_s,
    gated_s,
    bias_s,
    part_s,
    got_s,
    zpart_s,
    zgot_s,
    kv_sem,
    in_sem,
    late_sem,
    send_sem,
    recv_sem,
    zsend_sem,
    zrecv_sem,
):
    users, cands, block, heads, size, seqs, slices, local, out_cols = dims
    rows = heads * cands
    width = heads * size
    tiles = out_cols // LANES
    me = lax.axis_index("seq")
    mh = lax.axis_index("head")

    def landed(ref, sem):
        pltpu.make_async_copy(ref, ref, sem).wait()

    scale = LOG2E / math.sqrt(size)

    barrier = pltpu.get_barrier_semaphore()
    for step in range(1, seqs):
        pl.semaphore_signal(
            barrier, inc=1, device_id={"seq": partner(me, step, seqs)}, device_id_type=MESH
        )
    for step in range(1, slices):
        pl.semaphore_signal(
            barrier, inc=1, device_id={"head": partner(mh, step, slices)}, device_id_type=MESH
        )

    early = [
        pltpu.make_async_copy(source, target, in_sem.at[min(i, 4)])
        for i, (source, target) in enumerate(
            (
                (len_hbm, len_ref),
                (tb_hbm, tb_s),
                (ab_hbm, ab_s),
                (q_hbm, q_s),
                (bucket_hbm, event_s.at[0]),
                (action_hbm, event_s.at[1]),
            )
        )
    ]
    mine = pl.ds(me * local, local)
    late = [
        pltpu.make_async_copy(source, target, late_sem.at[min(i, 2)])
        for i, (source, target) in enumerate(
            (
                (gain_hbm, gain_s),
                (w_hbm, w_s),
                (nk_hbm.at[mine], mine_s.at[0]),
                (nv_hbm.at[mine], mine_s.at[1]),
                (gate_hbm.at[mine], mine_s.at[2]),
            )
        )
    ]
    for copy in early:
        copy.start()
    order = []
    groups = plan(seqs, local)
    for index, group in enumerate(groups):
        for turn, step in group:
            user = partner(me, step, seqs) * local + turn
            for part, source in enumerate((k_hbm, v_hbm)):
                pltpu.make_async_copy(
                    source.at[user], kv_s.at[len(order), part], kv_sem.at[index]
                ).start(priority=1)
            order.append((turn, step, user))
    for copy in late:
        copy.start()
    for copy in early[:4]:
        copy.wait()
    landed(event_s, in_sem.at[4])

    lane_of = lax.broadcasted_iota(jnp.int32, (users, cands, width), 2)
    query = q_s[...]
    for head in range(heads):
        qd_s[:, head * cands : (head + 1) * cands, :] = jnp.where(
            lane_of // size == head, query, jnp.zeros_like(query)
        )

    def table(ref, head):
        row = ref[head : head + 1, :] * LOG2E
        return jnp.concatenate([row, jnp.zeros((1, LANES - row.shape[1]), row.dtype)], axis=1)

    user_id = lax.broadcasted_iota(jnp.int32, (users, LANES), 0)
    limit = jnp.zeros((users, LANES), jnp.int32)
    for user in range(users):
        limit = jnp.where(user_id == user, len_ref[user], limit)
    limit = limit - me * block - lax.broadcasted_iota(jnp.int32, (users, LANES), 1)
    for head in range(heads):
        tb_row = jnp.broadcast_to(table(tb_s, head), (users, LANES))
        ab_row = jnp.broadcast_to(table(ab_s, head), (users, LANES))
        for chunk in range(block // LANES):
            lanes = slice(chunk * LANES, (chunk + 1) * LANES)
            bias = jnp.take_along_axis(tb_row, event_s[0, :, lanes], axis=1) + jnp.take_along_axis(
                ab_row, event_s[1, :, lanes], axis=1
            )
            bias_s[head, :, lanes] = jnp.where(limit > chunk * LANES, bias, INVALID)

    for copy in late[:2]:
        copy.wait()
    landed(mine_s, late_sem.at[2])
    gate = mine_s[2].astype(jnp.float32)
    gated_s[...] = gain_s[...].reshape(1, 1, width) * (gate / (1.0 + jnp.exp(-gate)))

    def by_head(source):
        return jnp.concatenate(
            [source[:, head * size : (head + 1) * size] for head in range(heads)], axis=0
        )

    def score(slot):
        turn, step, user = order[slot]
        raw = lax.dot_general(qd_s[user], kv_s[slot, 0], NT, preferred_element_type=jnp.float32)
        bias = jnp.concatenate(
            [
                jnp.broadcast_to(bias_s[head, pl.ds(user, 1), :], (cands, block))
                for head in range(heads)
            ],
            axis=0,
        )
        scores = raw * scale + bias
        top = jnp.maximum(jnp.max(scores, axis=1, keepdims=True), FLOOR)
        fresh = None
        if step == 0:
            product = q_s[user].astype(jnp.float32) * mine_s[0, turn].astype(jnp.float32)
            own = jnp.sum(by_head(product), axis=1, keepdims=True) * scale
            top = jnp.maximum(top, own)
            fresh = jnp.exp2(own - top)
        weights = jnp.exp2(scores - top)
        total = jnp.sum(weights, axis=1, keepdims=True)
        if step == 0:
            total = total + fresh
            fresh = fresh * by_head(mine_s[1, turn].astype(jnp.float32))
        stats = column_to_row(top, 0, size) + column_to_row(total, rows, size)
        part_s[turn, step, rows : rows + 1, :] = stats
        return weights.astype(jnp.bfloat16), fresh

    def mix(slot, weights, fresh):
        turn, step, _ = order[slot]
        mixed = jnp.dot(weights, kv_s[slot, 1], preferred_element_type=jnp.float32)
        for head in range(heads):
            held = slice(head * cands, (head + 1) * cands)
            piece = mixed[held, head * size : (head + 1) * size]
            part_s[turn, step, held, :] = piece if fresh is None else piece + fresh[held]

    def attend(slots):
        waiting = []
        for slot in slots:
            waiting.append((slot, *score(slot)))
            if len(waiting) > 1:
                mix(*waiting.pop(0))
        for item in waiting:
            mix(*item)

    def exchange(turn, step):
        return pltpu.make_async_remote_copy(
            src_ref=part_s.at[turn, step],
            dst_ref=got_s.at[turn, step - 1],
            send_sem=send_sem,
            recv_sem=recv_sem.at[turn],
            device_id={"seq": partner(me, step, seqs)},
            device_id_type=MESH,
        )

    def spread(turn, step):
        target = partner(mh, step, slices)
        return pltpu.make_async_remote_copy(
            src_ref=zpart_s.at[turn, target],
            dst_ref=zgot_s.at[turn, step - 1],
            send_sem=zsend_sem,
            recv_sem=zrecv_sem.at[turn],
            device_id={"head": target},
            device_id_type=MESH,
        )

    def combine(turn):
        landed(got_s.at[turn], recv_sem.at[turn])
        blocks = [part_s.at[turn, 0]] + [got_s.at[turn, step - 1] for step in range(1, seqs)]
        maxima = [row_to_column(ref[rows : rows + 1, :], 0, rows) for ref in blocks]
        sums = [row_to_column(ref[rows : rows + 1, :], rows, rows) for ref in blocks]
        top = functools.reduce(jnp.maximum, maxima)
        numer, denom = 0.0, 0.0
        for ref, high, amount in zip(blocks, maxima, sums):
            factor = jnp.exp2(high - top)
            numer = numer + factor * ref[:rows, :]
            denom = denom + factor * amount
        attended = numer / denom
        squares = jnp.sum(jnp.square(attended), axis=1, keepdims=True)
        square = squares[:cands]
        for head in range(1, heads):
            square = square + squares[head * cands : (head + 1) * cands]
        wide = jnp.concatenate(
            [attended[head * cands : (head + 1) * cands] for head in range(heads)], axis=1
        )
        hidden = (wide * gated_s[turn]).astype(jnp.bfloat16)
        projected = jnp.dot(hidden, w_s[...], preferred_element_type=jnp.float32)
        square_row = column_to_row(square, 0, LANES)
        for target in range(slices):
            for tile in range(tiles):
                first = target * out_cols + tile * LANES
                zpart_s[turn, target, tile * cands : (tile + 1) * cands, :] = projected[
                    :, first : first + LANES
                ]
            zpart_s[turn, target, tiles * cands : tiles * cands + 1, :] = square_row
        for step in range(slices - 1, 0, -1):
            spread(turn, step).start()

    def finish(turn):
        landed(zgot_s.at[turn], zrecv_sem.at[turn])
        total = zpart_s[turn, mh]
        for step in range(1, slices):
            total = total + zgot_s[turn, step - 1]
        column = row_to_column(total[tiles * cands :, :], 0, cands)
        factor = 1.0 / jnp.sqrt(column / (width * slices) + 1e-6)
        for tile in range(tiles):
            piece = total[tile * cands : (tile + 1) * cands] * factor
            out_ref[turn, :, tile * LANES : (tile + 1) * LANES] = piece.astype(out_ref.dtype)

    first = 0
    ready = {turn: 0 for turn in range(local)}
    done = 0
    for index, group in enumerate(groups):
        slots = list(range(first, first + len(group)))
        first += len(group)
        landed(kv_s.at[slots[0] : slots[-1] + 1], kv_sem.at[index])
        attend(slots)
        if index == 0:
            pl.semaphore_wait(barrier, seqs - 1 + slices - 1)
        for turn, step in group:
            ready[turn] += 1
            if step:
                exchange(turn, step).start()
        if first >= START * len(order) // 16 and ready[done] == seqs and index < len(groups) - 1:
            combine(done)
            done += 1
    while done < local:
        combine(done)
        done += 1
    for turn in range(local):
        finish(turn)
    landed(got_s, send_sem)
    landed(zgot_s, zsend_sem)


def body(
    query,
    new_key,
    new_value,
    keys,
    values,
    lengths,
    time_bucket,
    action,
    time_bias,
    action_bias,
    gate,
    norm_gain,
    w_out,
):
    users, block, width = keys.shape
    cands = query.shape[1]
    heads = time_bias.shape[1]
    size = width // heads
    seqs = lax.axis_size("seq")
    slices = lax.axis_size("head")
    local = users // seqs
    rows = heads * cands
    out_cols = w_out.shape[1] // slices
    tiles = out_cols // LANES
    groups = len(plan(seqs, local))
    dims = (users, cands, block, heads, size, seqs, slices, local, out_cols)
    f32, bf16 = jnp.float32, jnp.bfloat16
    anywhere = pl.BlockSpec(memory_space=pltpu.HBM)
    return pl.pallas_call(
        functools.partial(kernel, dims),
        out_shape=jax.ShapeDtypeStruct((local, cands, out_cols), bf16),
        in_specs=[anywhere] * 13,
        out_specs=pl.BlockSpec(memory_space=pltpu.VMEM),
        scratch_shapes=[
            pltpu.SMEM((users,), jnp.int32),
            pltpu.VMEM((users, cands, width), bf16),
            pltpu.VMEM((3, local, cands, width), bf16),
            pltpu.VMEM((users, 2, block, width), bf16),
            pltpu.VMEM((2, users, block), jnp.int32),
            pltpu.VMEM(time_bias.T.shape, f32),
            pltpu.VMEM(action_bias.T.shape, f32),
            pltpu.VMEM((width,), f32),
            pltpu.VMEM(w_out.shape, bf16),
            pltpu.VMEM((users, rows, width), bf16),
            pltpu.VMEM((local, cands, width), f32),
            pltpu.VMEM((heads, users, block), f32),
            pltpu.VMEM((local, seqs, rows + 1, size), f32),
            pltpu.VMEM((local, seqs - 1, rows + 1, size), f32),
            pltpu.VMEM((local, slices, tiles * cands + 1, LANES), f32),
            pltpu.VMEM((local, slices - 1, tiles * cands + 1, LANES), f32),
            pltpu.SemaphoreType.DMA((groups,)),
            pltpu.SemaphoreType.DMA((5,)),
            pltpu.SemaphoreType.DMA((3,)),
            pltpu.SemaphoreType.DMA,
            pltpu.SemaphoreType.DMA((local,)),
            pltpu.SemaphoreType.DMA,
            pltpu.SemaphoreType.DMA((local,)),
        ],
        compiler_params=pltpu.CompilerParams(
            collective_id=0, has_side_effects=True, vmem_limit_bytes=52428800
        ),
    )(
        *(
            pltpu.with_memory_space_constraint(x, pltpu.HBM)
            for x in (
                lengths,
                query,
                new_key,
                new_value,
                keys,
                values,
                time_bucket,
                action,
                time_bias.T,
                action_bias.T,
                gate,
                norm_gain,
                w_out,
            )
        )
    )


def solution(mesh):
    placed = (
        P("groups", None, "head"),
        P("groups", None, "head"),
        P("groups", None, "head"),
        P("groups", "seq", "head"),
        P("groups", "seq", "head"),
        P("groups"),
        P("groups", "seq"),
        P("groups", "seq"),
        P(None, "head"),
        P(None, "head"),
        P("groups", None, "head"),
        P("head"),
        P("head", None),
    )
    return jax.shard_map(
        body,
        mesh=mesh,
        in_specs=placed,
        out_specs=P(("groups", "seq"), None, "head"),
        check_vma=False,
    )
```

```python
import functools
import math

import jax
import jax.numpy as jnp
from jax import lax
from jax.experimental import pallas as pl
from jax.experimental.pallas import tpu as pltpu
from jax.sharding import PartitionSpec as P

MESH = pl.DeviceIdType.MESH
LANES = 128
LOG2E = math.log2(math.e)
GROUP = 3
START = 11
INVALID = -1e30
FLOOR = -1e29
NT = (((1,), (1,)), ((), ()))


def partner(rank, step, count):
    result, bit = 0, 1
    while bit < count:
        held = (rank // bit) % 2
        result = result + bit * (1 - held if (step // bit) % 2 else held)
        bit *= 2
    return result


def plan(seqs, local):
    far = range(seqs - 1, 1, -1)
    near = [step for step in (1, 0) if step < seqs]
    order = [(0, step) for step in far]
    for turn in range(1, local):
        if near and turn <= len(near):
            order.append((0, near[turn - 1]))
        order += [(turn, step) for step in far]
    order += [(0, step) for step in near[max(local - 1, 0) :]]
    order += [(turn, step) for step in near for turn in range(1, local)]
    groups, first = [], 0
    while first < len(order):
        size = GROUP if first else GROUP - 1
        groups.append(order[first : first + size])
        first += size
    acts, taken, ready, done = [], 0, [0] * local, 0
    for group in groups:
        acts.append(group)
        taken += len(group)
        for turn, _ in group:
            ready[turn] += 1
        if taken < len(order) and 16 * taken >= START * len(order) and ready[done] == seqs:
            acts.append(done)
            done += 1
    return acts + list(range(done, local))


def column_to_row(column, first, lanes):
    shape = (column.shape[0], lanes)
    row_id = lax.broadcasted_iota(jnp.int32, shape, 0)
    lane_id = lax.broadcasted_iota(jnp.int32, shape, 1)
    return jnp.sum(jnp.where(lane_id == row_id + first, column, 0.0), axis=0, keepdims=True)


def row_to_column(row, first, count):
    shape = (count, row.shape[1])
    row_id = lax.broadcasted_iota(jnp.int32, shape, 0)
    lane_id = lax.broadcasted_iota(jnp.int32, shape, 1)
    return jnp.sum(jnp.where(lane_id == row_id + first, row, 0.0), axis=1, keepdims=True)


def kernel(
    dims,
    len_hbm,
    q_hbm,
    nk_hbm,
    nv_hbm,
    k_hbm,
    v_hbm,
    bucket_hbm,
    action_hbm,
    tb_hbm,
    ab_hbm,
    gate_hbm,
    gain_hbm,
    w_hbm,
    out_ref,
    len_ref,
    q_s,
    mine_s,
    kv_s,
    event_s,
    tb_s,
    ab_s,
    gain_s,
    w_s,
    qd_s,
    gated_s,
    bias_s,
    part_s,
    got_s,
    zpart_s,
    zgot_s,
    kv_sem,
    in_sem,
    late_sem,
    send_sem,
    recv_sem,
    zsend_sem,
    zrecv_sem,
):
    users, cands, block, heads, size, seqs, slices, local, out_cols = dims
    rows = heads * cands
    width = heads * size
    tiles = out_cols // LANES
    me = lax.axis_index("seq")
    mh = lax.axis_index("head")

    def landed(ref, sem):
        pltpu.make_async_copy(ref, ref, sem).wait()

    scale = LOG2E / math.sqrt(size)

    barrier = pltpu.get_barrier_semaphore()
    for step in range(1, seqs):
        pl.semaphore_signal(
            barrier, inc=1, device_id={"seq": partner(me, step, seqs)}, device_id_type=MESH
        )
    for step in range(1, slices):
        pl.semaphore_signal(
            barrier, inc=1, device_id={"head": partner(mh, step, slices)}, device_id_type=MESH
        )

    early = [
        pltpu.make_async_copy(source, target, in_sem.at[min(i, 4)])
        for i, (source, target) in enumerate(
            (
                (len_hbm, len_ref),
                (tb_hbm, tb_s),
                (ab_hbm, ab_s),
                (q_hbm, q_s),
                (bucket_hbm, event_s.at[0]),
                (action_hbm, event_s.at[1]),
            )
        )
    ]
    mine = pl.ds(me * local, local)
    late = [
        pltpu.make_async_copy(source, target, late_sem.at[min(i, 2)])
        for i, (source, target) in enumerate(
            (
                (gain_hbm, gain_s),
                (w_hbm, w_s),
                (nk_hbm.at[mine], mine_s.at[0]),
                (nv_hbm.at[mine], mine_s.at[1]),
                (gate_hbm.at[mine], mine_s.at[2]),
            )
        )
    ]
    for copy in early:
        copy.start()
    order = []
    acts = plan(seqs, local)
    groups = [act for act in acts if isinstance(act, list)]
    starts = [sum(len(group) for group in groups[:index]) for index in range(len(groups))]
    for index, group in enumerate(groups):
        for turn, step in group:
            user = partner(me, step, seqs) * local + turn
            for part, source in enumerate((k_hbm, v_hbm)):
                pltpu.make_async_copy(
                    source.at[user], kv_s.at[len(order), part], kv_sem.at[index]
                ).start(priority=1)
            order.append((turn, step, user))
    for copy in late:
        copy.start()
    for copy in early[:4]:
        copy.wait()
    landed(event_s, in_sem.at[4])

    lane_of = lax.broadcasted_iota(jnp.int32, (users, cands, width), 2)
    query = q_s[...]
    for head in range(heads):
        qd_s[:, head * cands : (head + 1) * cands, :] = jnp.where(
            lane_of // size == head, query, jnp.zeros_like(query)
        )

    def table(ref, head):
        row = ref[head : head + 1, :] * LOG2E
        return jnp.concatenate([row, jnp.zeros((1, LANES - row.shape[1]), row.dtype)], axis=1)

    user_id = lax.broadcasted_iota(jnp.int32, (users, LANES), 0)
    limit = jnp.zeros((users, LANES), jnp.int32)
    for user in range(users):
        limit = jnp.where(user_id == user, len_ref[user], limit)
    limit = limit - me * block - lax.broadcasted_iota(jnp.int32, (users, LANES), 1)
    for head in range(heads):
        tb_row = jnp.broadcast_to(table(tb_s, head), (users, LANES))
        ab_row = jnp.broadcast_to(table(ab_s, head), (users, LANES))
        for chunk in range(block // LANES):
            lanes = slice(chunk * LANES, (chunk + 1) * LANES)
            bias = jnp.take_along_axis(tb_row, event_s[0, :, lanes], axis=1) + jnp.take_along_axis(
                ab_row, event_s[1, :, lanes], axis=1
            )
            bias_s[head, :, lanes] = jnp.where(limit > chunk * LANES, bias, INVALID)

    for copy in late[:2]:
        copy.wait()
    landed(mine_s, late_sem.at[2])
    gate = mine_s[2].astype(jnp.float32)
    gated_s[...] = gain_s[...].reshape(1, 1, width) * (gate / (1.0 + jnp.exp(-gate)))

    def by_head(source):
        return jnp.concatenate(
            [source[:, head * size : (head + 1) * size] for head in range(heads)], axis=0
        )

    def score(slot):
        turn, step, user = order[slot]
        raw = lax.dot_general(qd_s[user], kv_s[slot, 0], NT, preferred_element_type=jnp.float32)
        bias = jnp.concatenate(
            [
                jnp.broadcast_to(bias_s[head, pl.ds(user, 1), :], (cands, block))
                for head in range(heads)
            ],
            axis=0,
        )
        scores = raw * scale + bias
        top = jnp.maximum(jnp.max(scores, axis=1, keepdims=True), FLOOR)
        fresh = None
        if step == 0:
            product = q_s[user].astype(jnp.float32) * mine_s[0, turn].astype(jnp.float32)
            own = jnp.sum(by_head(product), axis=1, keepdims=True) * scale
            top = jnp.maximum(top, own)
            fresh = jnp.exp2(own - top)
        weights = jnp.exp2(scores - top)
        total = jnp.sum(weights, axis=1, keepdims=True)
        if step == 0:
            total = total + fresh
            fresh = fresh * by_head(mine_s[1, turn].astype(jnp.float32))
        stats = column_to_row(top, 0, size) + column_to_row(total, rows, size)
        part_s[turn, step, rows : rows + 1, :] = stats
        return weights.astype(jnp.bfloat16), fresh

    def mix(slot, weights, fresh):
        turn, step, _ = order[slot]
        mixed = jnp.dot(weights, kv_s[slot, 1], preferred_element_type=jnp.float32)
        for head in range(heads):
            held = slice(head * cands, (head + 1) * cands)
            piece = mixed[held, head * size : (head + 1) * size]
            part_s[turn, step, held, :] = piece if fresh is None else piece + fresh[held]

    def exchange(turn, step):
        return pltpu.make_async_remote_copy(
            src_ref=part_s.at[turn, step],
            dst_ref=got_s.at[turn, step - 1],
            send_sem=send_sem,
            recv_sem=recv_sem.at[turn],
            device_id={"seq": partner(me, step, seqs)},
            device_id_type=MESH,
        )

    def spread(turn, step):
        target = partner(mh, step, slices)
        return pltpu.make_async_remote_copy(
            src_ref=zpart_s.at[turn, target],
            dst_ref=zgot_s.at[turn, step - 1],
            send_sem=zsend_sem,
            recv_sem=zrecv_sem.at[turn],
            device_id={"head": target},
            device_id_type=MESH,
        )

    def combine(turn):
        landed(got_s.at[turn], recv_sem.at[turn])
        blocks = [part_s.at[turn, 0]] + [got_s.at[turn, step - 1] for step in range(1, seqs)]
        maxima = [row_to_column(ref[rows : rows + 1, :], 0, rows) for ref in blocks]
        sums = [row_to_column(ref[rows : rows + 1, :], rows, rows) for ref in blocks]
        top = functools.reduce(jnp.maximum, maxima)
        numer, denom = 0.0, 0.0
        for ref, high, amount in zip(blocks, maxima, sums):
            factor = jnp.exp2(high - top)
            numer = numer + factor * ref[:rows, :]
            denom = denom + factor * amount
        attended = numer / denom
        squares = jnp.sum(jnp.square(attended), axis=1, keepdims=True)
        square = squares[:cands]
        for head in range(1, heads):
            square = square + squares[head * cands : (head + 1) * cands]
        wide = jnp.concatenate(
            [attended[head * cands : (head + 1) * cands] for head in range(heads)], axis=1
        )
        hidden = (wide * gated_s[turn]).astype(jnp.bfloat16)
        projected = jnp.dot(hidden, w_s[...], preferred_element_type=jnp.float32)
        square_row = column_to_row(square, 0, LANES)
        for target in range(slices):
            for tile in range(tiles):
                first = target * out_cols + tile * LANES
                zpart_s[turn, target, tile * cands : (tile + 1) * cands, :] = projected[
                    :, first : first + LANES
                ]
            zpart_s[turn, target, tiles * cands : tiles * cands + 1, :] = square_row
        for step in range(slices - 1, 0, -1):
            spread(turn, step).start()

    def finish(turn):
        landed(zgot_s.at[turn], zrecv_sem.at[turn])
        total = zpart_s[turn, mh]
        for step in range(1, slices):
            total = total + zgot_s[turn, step - 1]
        column = row_to_column(total[tiles * cands :, :], 0, cands)
        factor = 1.0 / jnp.sqrt(column / (width * slices) + 1e-6)
        for tile in range(tiles):
            piece = total[tile * cands : (tile + 1) * cands] * factor
            out_ref[turn, :, tile * LANES : (tile + 1) * LANES] = piece.astype(out_ref.dtype)

    index = 0
    for act in acts:
        if isinstance(act, int):
            combine(act)
            continue
        first, last = starts[index], starts[index] + len(act)
        landed(kv_s.at[first:last], kv_sem.at[index])
        waiting = []
        for slot in range(first, last):
            waiting.append((slot, *score(slot)))
            if len(waiting) > 1:
                mix(*waiting.pop(0))
        mix(*waiting.pop(0))
        if index == 0:
            pl.semaphore_wait(barrier, seqs - 1 + slices - 1)
        for turn, step in act:
            if step:
                exchange(turn, step).start()
        index += 1
    for turn in range(local):
        finish(turn)
    landed(got_s, send_sem)
    landed(zgot_s, zsend_sem)


def body(
    query,
    new_key,
    new_value,
    keys,
    values,
    lengths,
    time_bucket,
    action,
    time_bias,
    action_bias,
    gate,
    norm_gain,
    w_out,
):
    users, block, width = keys.shape
    cands = query.shape[1]
    heads = time_bias.shape[1]
    size = width // heads
    seqs = lax.axis_size("seq")
    slices = lax.axis_size("head")
    local = users // seqs
    rows = heads * cands
    out_cols = w_out.shape[1] // slices
    tiles = out_cols // LANES
    groups = len([act for act in plan(seqs, local) if isinstance(act, list)])
    dims = (users, cands, block, heads, size, seqs, slices, local, out_cols)
    f32, bf16 = jnp.float32, jnp.bfloat16
    anywhere = pl.BlockSpec(memory_space=pltpu.HBM)
    return pl.pallas_call(
        functools.partial(kernel, dims),
        out_shape=jax.ShapeDtypeStruct((local, cands, out_cols), bf16),
        in_specs=[anywhere] * 13,
        out_specs=pl.BlockSpec(memory_space=pltpu.VMEM),
        scratch_shapes=[
            pltpu.SMEM((users,), jnp.int32),
            pltpu.VMEM((users, cands, width), bf16),
            pltpu.VMEM((3, local, cands, width), bf16),
            pltpu.VMEM((users, 2, block, width), bf16),
            pltpu.VMEM((2, users, block), jnp.int32),
            pltpu.VMEM(time_bias.T.shape, f32),
            pltpu.VMEM(action_bias.T.shape, f32),
            pltpu.VMEM((width,), f32),
            pltpu.VMEM(w_out.shape, bf16),
            pltpu.VMEM((users, rows, width), bf16),
            pltpu.VMEM((local, cands, width), f32),
            pltpu.VMEM((heads, users, block), f32),
            pltpu.VMEM((local, seqs, rows + 1, size), f32),
            pltpu.VMEM((local, seqs - 1, rows + 1, size), f32),
            pltpu.VMEM((local, slices, tiles * cands + 1, LANES), f32),
            pltpu.VMEM((local, slices - 1, tiles * cands + 1, LANES), f32),
            pltpu.SemaphoreType.DMA((groups,)),
            pltpu.SemaphoreType.DMA((5,)),
            pltpu.SemaphoreType.DMA((3,)),
            pltpu.SemaphoreType.DMA,
            pltpu.SemaphoreType.DMA((local,)),
            pltpu.SemaphoreType.DMA,
            pltpu.SemaphoreType.DMA((local,)),
        ],
        compiler_params=pltpu.CompilerParams(
            collective_id=0, has_side_effects=True, vmem_limit_bytes=52428800
        ),
    )(
        *(
            pltpu.with_memory_space_constraint(x, pltpu.HBM)
            for x in (
                lengths,
                query,
                new_key,
                new_value,
                keys,
                values,
                time_bucket,
                action,
                time_bias.T,
                action_bias.T,
                gate,
                norm_gain,
                w_out,
            )
        )
    )


def solution(mesh):
    placed = (
        P("groups", None, "head"),
        P("groups", None, "head"),
        P("groups", None, "head"),
        P("groups", "seq", "head"),
        P("groups", "seq", "head"),
        P("groups"),
        P("groups", "seq"),
        P("groups", "seq"),
        P(None, "head"),
        P(None, "head"),
        P("groups", None, "head"),
        P("head"),
        P("head", None),
    )
    return jax.shard_map(
        body,
        mesh=mesh,
        in_specs=placed,
        out_specs=P(("groups", "seq"), None, "head"),
        check_vma=False,
    )
```

```python
import functools
import math

import jax
import jax.numpy as jnp
from jax import lax
from jax.experimental import pallas as pl
from jax.experimental.pallas import tpu as pltpu
from jax.sharding import PartitionSpec as P

MESH = pl.DeviceIdType.MESH
LANES = 128
LOG2E = math.log2(math.e)
GROUP = 3
SIZES = [2, 3, 4, 2]
START = 11
DEFER = 2
INVALID = -1e30
FLOOR = -1e29
NT = (((1,), (1,)), ((), ()))


def partner(rank, step, count):
    result, bit = 0, 1
    while bit < count:
        held = (rank // bit) % 2
        result = result + bit * (1 - held if (step // bit) % 2 else held)
        bit *= 2
    return result


def plan(seqs, local):
    far = range(2, seqs)
    near = [step for step in (1, 0) if step < seqs]
    order = [(turn, step) for turn in range(min(local, 2)) for step in far]
    order += [(0, step) for step in near[:-1]]
    order += [(turn, step) for turn in range(2, local) for step in far]
    order += [(0, step) for step in near[-1:]]
    order += [(turn, step) for step in near for turn in range(1, local)]
    groups, first = [], 0
    for size in SIZES + [GROUP] * len(order):
        if first < len(order):
            groups.append(order[first : first + size])
            first += size
    acts, taken, ready, done = [], 0, [0] * local, 0
    for group in groups:
        acts.append(group)
        taken += len(group)
        for turn, _ in group:
            ready[turn] += 1
        if taken < len(order) and 16 * taken >= START * len(order) and ready[done] == seqs:
            acts.append(done)
            done += 1
    return acts + list(range(done, local))


def column_to_row(column, first, lanes):
    shape = (column.shape[0], lanes)
    row_id = lax.broadcasted_iota(jnp.int32, shape, 0)
    lane_id = lax.broadcasted_iota(jnp.int32, shape, 1)
    return jnp.sum(jnp.where(lane_id == row_id + first, column, 0.0), axis=0, keepdims=True)


def row_to_column(row, first, count):
    shape = (count, row.shape[1])
    row_id = lax.broadcasted_iota(jnp.int32, shape, 0)
    lane_id = lax.broadcasted_iota(jnp.int32, shape, 1)
    return jnp.sum(jnp.where(lane_id == row_id + first, row, 0.0), axis=1, keepdims=True)


def kernel(
    dims,
    len_hbm,
    q_hbm,
    nk_hbm,
    nv_hbm,
    k_hbm,
    v_hbm,
    bucket_hbm,
    action_hbm,
    tb_hbm,
    ab_hbm,
    gate_hbm,
    gain_hbm,
    w_hbm,
    out_ref,
    len_ref,
    q_s,
    mine_s,
    kv_s,
    event_s,
    tb_s,
    ab_s,
    gain_s,
    w_s,
    qd_s,
    gated_s,
    bias_s,
    part_s,
    got_s,
    zpart_s,
    zgot_s,
    kv_sem,
    in_sem,
    late_sem,
    send_sem,
    recv_sem,
    zsend_sem,
    zrecv_sem,
):
    users, cands, block, heads, size, seqs, slices, local, out_cols = dims
    rows = heads * cands
    width = heads * size
    tiles = out_cols // LANES
    me = lax.axis_index("seq")
    mh = lax.axis_index("head")

    def landed(ref, sem):
        pltpu.make_async_copy(ref, ref, sem).wait()

    scale = LOG2E / math.sqrt(size)

    barrier = pltpu.get_barrier_semaphore()
    for step in range(1, seqs):
        pl.semaphore_signal(
            barrier, inc=1, device_id={"seq": partner(me, step, seqs)}, device_id_type=MESH
        )
    for step in range(1, slices):
        pl.semaphore_signal(
            barrier, inc=1, device_id={"head": partner(mh, step, slices)}, device_id_type=MESH
        )

    early = [
        pltpu.make_async_copy(source, target, in_sem.at[min(i, 4)])
        for i, (source, target) in enumerate(
            (
                (len_hbm, len_ref),
                (tb_hbm, tb_s),
                (ab_hbm, ab_s),
                (q_hbm, q_s),
                (bucket_hbm, event_s.at[0]),
                (action_hbm, event_s.at[1]),
            )
        )
    ]
    mine = pl.ds(me * local, local)
    late = [
        pltpu.make_async_copy(source, target, late_sem.at[min(i, 2)])
        for i, (source, target) in enumerate(
            (
                (gain_hbm, gain_s),
                (w_hbm, w_s),
                (nk_hbm.at[mine], mine_s.at[0]),
                (nv_hbm.at[mine], mine_s.at[1]),
                (gate_hbm.at[mine], mine_s.at[2]),
            )
        )
    ]
    for copy in early:
        copy.start()
    order = []
    acts = plan(seqs, local)
    groups = [act for act in acts if isinstance(act, list)]
    starts = [sum(len(group) for group in groups[:index]) for index in range(len(groups))]
    for index, group in enumerate(groups):
        for turn, step in group:
            user = partner(me, step, seqs) * local + turn
            for part, source in enumerate((k_hbm, v_hbm)):
                pltpu.make_async_copy(
                    source.at[user], kv_s.at[len(order), part], kv_sem.at[index]
                ).start(priority=1)
            order.append((turn, step, user))
    for copy in late:
        copy.start()
    for copy in early[:4]:
        copy.wait()
    landed(event_s, in_sem.at[4])

    lane_of = lax.broadcasted_iota(jnp.int32, (users, cands, width), 2)
    query = q_s[...]
    for head in range(heads):
        qd_s[:, head * cands : (head + 1) * cands, :] = jnp.where(
            lane_of // size == head, query, jnp.zeros_like(query)
        )

    def table(ref, head):
        row = ref[head : head + 1, :] * LOG2E
        return jnp.concatenate([row, jnp.zeros((1, LANES - row.shape[1]), row.dtype)], axis=1)

    user_id = lax.broadcasted_iota(jnp.int32, (users, LANES), 0)
    limit = jnp.zeros((users, LANES), jnp.int32)
    for user in range(users):
        limit = jnp.where(user_id == user, len_ref[user], limit)
    limit = limit - me * block - lax.broadcasted_iota(jnp.int32, (users, LANES), 1)
    for head in range(heads):
        tb_row = jnp.broadcast_to(table(tb_s, head), (users, LANES))
        ab_row = jnp.broadcast_to(table(ab_s, head), (users, LANES))
        for chunk in range(block // LANES):
            lanes = slice(chunk * LANES, (chunk + 1) * LANES)
            bias = jnp.take_along_axis(tb_row, event_s[0, :, lanes], axis=1) + jnp.take_along_axis(
                ab_row, event_s[1, :, lanes], axis=1
            )
            bias_s[head, :, lanes] = jnp.where(limit > chunk * LANES, bias, INVALID)

    for copy in late[:2]:
        copy.wait()
    landed(mine_s, late_sem.at[2])
    gate = mine_s[2].astype(jnp.float32)
    gated_s[...] = gain_s[...].reshape(1, 1, width) * (gate / (1.0 + jnp.exp(-gate)))

    def by_head(source):
        return jnp.concatenate(
            [source[:, head * size : (head + 1) * size] for head in range(heads)], axis=0
        )

    def score(slot):
        turn, step, user = order[slot]
        raw = lax.dot_general(qd_s[user], kv_s[slot, 0], NT, preferred_element_type=jnp.float32)
        bias = jnp.concatenate(
            [
                jnp.broadcast_to(bias_s[head, pl.ds(user, 1), :], (cands, block))
                for head in range(heads)
            ],
            axis=0,
        )
        scores = raw * scale + bias
        top = jnp.maximum(jnp.max(scores, axis=1, keepdims=True), FLOOR)
        fresh = None
        if step == 0:
            product = q_s[user].astype(jnp.float32) * mine_s[0, turn].astype(jnp.float32)
            own = jnp.sum(by_head(product), axis=1, keepdims=True) * scale
            top = jnp.maximum(top, own)
            fresh = jnp.exp2(own - top)
        weights = jnp.exp2(scores - top)
        total = jnp.sum(weights, axis=1, keepdims=True)
        if step == 0:
            total = total + fresh
            fresh = fresh * by_head(mine_s[1, turn].astype(jnp.float32))
        stats = column_to_row(top, 0, size) + column_to_row(total, rows, size)
        part_s[turn, step, rows : rows + 1, :] = stats
        return weights.astype(jnp.bfloat16), fresh

    def mix(slot, weights, fresh):
        turn, step, _ = order[slot]
        mixed = jnp.dot(weights, kv_s[slot, 1], preferred_element_type=jnp.float32)
        for head in range(heads):
            held = slice(head * cands, (head + 1) * cands)
            piece = mixed[held, head * size : (head + 1) * size]
            part_s[turn, step, held, :] = piece if fresh is None else piece + fresh[held]

    def exchange(turn, step):
        return pltpu.make_async_remote_copy(
            src_ref=part_s.at[turn, step],
            dst_ref=got_s.at[turn, step - 1],
            send_sem=send_sem,
            recv_sem=recv_sem.at[turn],
            device_id={"seq": partner(me, step, seqs)},
            device_id_type=MESH,
        )

    def receiver(rank):
        first = (slices - mh) // slices
        if rank == 0:
            return first * (slices - 1)
        below = slices - rank - 1
        return below + (below - mh - first * slices + 2 * slices) // (2 * slices)

    def spread(turn, rank):
        target = receiver(rank)
        return pltpu.make_async_remote_copy(
            src_ref=zpart_s.at[turn, target],
            dst_ref=zgot_s.at[turn, mh - (mh - target - 1 + slices) // slices],
            send_sem=zsend_sem,
            recv_sem=zrecv_sem.at[turn],
            device_id={"head": target},
            device_id_type=MESH,
        )

    later = []

    def combine(turn):
        landed(got_s.at[turn], recv_sem.at[turn])
        blocks = [part_s.at[turn, 0]] + [got_s.at[turn, step - 1] for step in range(1, seqs)]
        maxima = [row_to_column(ref[rows : rows + 1, :], 0, rows) for ref in blocks]
        sums = [row_to_column(ref[rows : rows + 1, :], rows, rows) for ref in blocks]
        top = functools.reduce(jnp.maximum, maxima)
        numer, denom = 0.0, 0.0
        for ref, high, amount in zip(blocks, maxima, sums):
            factor = jnp.exp2(high - top)
            numer = numer + factor * ref[:rows, :]
            denom = denom + factor * amount
        attended = numer / denom
        squares = jnp.sum(jnp.square(attended), axis=1, keepdims=True)
        square = squares[:cands]
        for head in range(1, heads):
            square = square + squares[head * cands : (head + 1) * cands]
        wide = jnp.concatenate(
            [attended[head * cands : (head + 1) * cands] for head in range(heads)], axis=1
        )
        hidden = (wide * gated_s[turn]).astype(jnp.bfloat16)
        projected = jnp.dot(hidden, w_s[...], preferred_element_type=jnp.float32)
        square_row = column_to_row(square, 0, LANES)
        for target in range(slices):
            for tile in range(tiles):
                first = target * out_cols + tile * LANES
                zpart_s[turn, target, tile * cands : (tile + 1) * cands, :] = projected[
                    :, first : first + LANES
                ]
            zpart_s[turn, target, tiles * cands : tiles * cands + 1, :] = square_row
        spread(turn, 0).start()
        later.append(turn)
        if turn == local - 1 or turn < local - DEFER:
            for held in later:
                for rank in range(1, slices - 1):
                    spread(held, rank).start()
            later.clear()

    def finish(turn):
        landed(zgot_s.at[turn], zrecv_sem.at[turn])
        total = zpart_s[turn, mh]
        for step in range(1, slices):
            total = total + zgot_s[turn, step - 1]
        column = row_to_column(total[tiles * cands :, :], 0, cands)
        factor = 1.0 / jnp.sqrt(column / (width * slices) + 1e-6)
        for tile in range(tiles):
            piece = total[tile * cands : (tile + 1) * cands] * factor
            out_ref[turn, :, tile * LANES : (tile + 1) * LANES] = piece.astype(out_ref.dtype)

    index = 0
    for act in acts:
        if isinstance(act, int):
            combine(act)
            continue
        first, last = starts[index], starts[index] + len(act)
        landed(kv_s.at[first:last], kv_sem.at[index])
        waiting = []
        for slot in range(first, last):
            waiting.append((slot, *score(slot)))
            if len(waiting) > 1:
                mix(*waiting.pop(0))
        mix(*waiting.pop(0))
        if index == 0:
            pl.semaphore_wait(barrier, seqs - 1 + slices - 1)
        for turn, step in act:
            if step:
                exchange(turn, step).start()
        index += 1
    for turn in range(local):
        finish(turn)
    landed(got_s, send_sem)
    landed(zgot_s, zsend_sem)


def body(
    query,
    new_key,
    new_value,
    keys,
    values,
    lengths,
    time_bucket,
    action,
    time_bias,
    action_bias,
    gate,
    norm_gain,
    w_out,
):
    users, block, width = keys.shape
    cands = query.shape[1]
    heads = time_bias.shape[1]
    size = width // heads
    seqs = lax.axis_size("seq")
    slices = lax.axis_size("head")
    local = users // seqs
    rows = heads * cands
    out_cols = w_out.shape[1] // slices
    tiles = out_cols // LANES
    groups = len([act for act in plan(seqs, local) if isinstance(act, list)])
    dims = (users, cands, block, heads, size, seqs, slices, local, out_cols)
    f32, bf16 = jnp.float32, jnp.bfloat16
    anywhere = pl.BlockSpec(memory_space=pltpu.HBM)
    return pl.pallas_call(
        functools.partial(kernel, dims),
        out_shape=jax.ShapeDtypeStruct((local, cands, out_cols), bf16),
        in_specs=[anywhere] * 13,
        out_specs=pl.BlockSpec(memory_space=pltpu.VMEM),
        scratch_shapes=[
            pltpu.SMEM((users,), jnp.int32),
            pltpu.VMEM((users, cands, width), bf16),
            pltpu.VMEM((3, local, cands, width), bf16),
            pltpu.VMEM((users, 2, block, width), bf16),
            pltpu.VMEM((2, users, block), jnp.int32),
            pltpu.VMEM(time_bias.T.shape, f32),
            pltpu.VMEM(action_bias.T.shape, f32),
            pltpu.VMEM((width,), f32),
            pltpu.VMEM(w_out.shape, bf16),
            pltpu.VMEM((users, rows, width), bf16),
            pltpu.VMEM((local, cands, width), f32),
            pltpu.VMEM((heads, users, block), f32),
            pltpu.VMEM((local, seqs, rows + 1, size), f32),
            pltpu.VMEM((local, seqs - 1, rows + 1, size), f32),
            pltpu.VMEM((local, slices, tiles * cands + 1, LANES), f32),
            pltpu.VMEM((local, slices - 1, tiles * cands + 1, LANES), f32),
            pltpu.SemaphoreType.DMA((groups,)),
            pltpu.SemaphoreType.DMA((5,)),
            pltpu.SemaphoreType.DMA((3,)),
            pltpu.SemaphoreType.DMA,
            pltpu.SemaphoreType.DMA((local,)),
            pltpu.SemaphoreType.DMA,
            pltpu.SemaphoreType.DMA((local,)),
        ],
        compiler_params=pltpu.CompilerParams(
            collective_id=0, has_side_effects=True, vmem_limit_bytes=52428800
        ),
    )(
        *(
            pltpu.with_memory_space_constraint(x, pltpu.HBM)
            for x in (
                lengths,
                query,
                new_key,
                new_value,
                keys,
                values,
                time_bucket,
                action,
                time_bias.T,
                action_bias.T,
                gate,
                norm_gain,
                w_out,
            )
        )
    )


def solution(mesh):
    placed = (
        P("groups", None, "head"),
        P("groups", None, "head"),
        P("groups", None, "head"),
        P("groups", "seq", "head"),
        P("groups", "seq", "head"),
        P("groups"),
        P("groups", "seq"),
        P("groups", "seq"),
        P(None, "head"),
        P(None, "head"),
        P("groups", None, "head"),
        P("head"),
        P("head", None),
    )
    return jax.shard_map(
        body,
        mesh=mesh,
        in_specs=placed,
        out_specs=P(("groups", "seq"), None, "head"),
        check_vma=False,
    )
```

```python
import functools
import math

import jax
import jax.numpy as jnp
from jax import lax
from jax.experimental import pallas as pl
from jax.experimental.pallas import tpu as pltpu
from jax.sharding import PartitionSpec as P

MESH = pl.DeviceIdType.MESH
LANES = 128
LOG2E = math.log2(math.e)
GROUP = 3
SIZES = [2, 3, 4, 2]
START = 11
DEFER = 2
WHEN = 4
INVALID = -1e30
FLOOR = -1e29
NT = (((1,), (1,)), ((), ()))


def partner(rank, step, count):
    result, bit = 0, 1
    while bit < count:
        held = (rank // bit) % 2
        result = result + bit * (1 - held if (step // bit) % 2 else held)
        bit *= 2
    return result


def plan(seqs, local):
    far = range(2, seqs)
    near = [step for step in (1, 0) if step < seqs]
    order = [(turn, step) for turn in range(min(local, 2)) for step in far]
    order += [(0, step) for step in near[:-1]]
    order += [(turn, step) for turn in range(2, local) for step in far]
    order += [(0, step) for step in near[-1:]]
    order += [(turn, step) for step in near for turn in range(1, local)]
    groups, first = [], 0
    for size in SIZES + [GROUP] * len(order):
        if first < len(order):
            groups.append(order[first : first + size])
            first += size
    acts, taken, ready, done = [], 0, [0] * local, 0
    for group in groups:
        acts.append(group)
        taken += len(group)
        for turn, _ in group:
            ready[turn] += 1
        if taken < len(order) and 16 * taken >= START * len(order) and ready[done] == seqs:
            acts.append(done)
            done += 1
    return acts + list(range(done, local))


def column_to_row(column, first, lanes):
    shape = (column.shape[0], lanes)
    row_id = lax.broadcasted_iota(jnp.int32, shape, 0)
    lane_id = lax.broadcasted_iota(jnp.int32, shape, 1)
    return jnp.sum(jnp.where(lane_id == row_id + first, column, 0.0), axis=0, keepdims=True)


def row_to_column(row, first, count):
    shape = (count, row.shape[1])
    row_id = lax.broadcasted_iota(jnp.int32, shape, 0)
    lane_id = lax.broadcasted_iota(jnp.int32, shape, 1)
    return jnp.sum(jnp.where(lane_id == row_id + first, row, 0.0), axis=1, keepdims=True)


def kernel(
    dims,
    len_hbm,
    q_hbm,
    nk_hbm,
    nv_hbm,
    k_hbm,
    v_hbm,
    bucket_hbm,
    action_hbm,
    tb_hbm,
    ab_hbm,
    gate_hbm,
    gain_hbm,
    w_hbm,
    out_ref,
    len_ref,
    q_s,
    mine_s,
    kv_s,
    event_s,
    tb_s,
    ab_s,
    gain_s,
    w_s,
    qd_s,
    gated_s,
    bias_s,
    part_s,
    got_s,
    zpart_s,
    zgot_s,
    kv_sem,
    in_sem,
    late_sem,
    send_sem,
    recv_sem,
    zsend_sem,
    zrecv_sem,
):
    users, cands, block, heads, size, seqs, slices, local, out_cols = dims
    rows = heads * cands
    width = heads * size
    tiles = out_cols // LANES
    me = lax.axis_index("seq")
    mh = lax.axis_index("head")

    def landed(ref, sem):
        pltpu.make_async_copy(ref, ref, sem).wait()

    scale = LOG2E / math.sqrt(size)

    barrier = pltpu.get_barrier_semaphore()
    for step in range(1, seqs):
        pl.semaphore_signal(
            barrier, inc=1, device_id={"seq": partner(me, step, seqs)}, device_id_type=MESH
        )
    for step in range(1, slices):
        pl.semaphore_signal(
            barrier, inc=1, device_id={"head": partner(mh, step, slices)}, device_id_type=MESH
        )

    early = [
        pltpu.make_async_copy(source, target, in_sem.at[min(i, 4)])
        for i, (source, target) in enumerate(
            (
                (len_hbm, len_ref),
                (tb_hbm, tb_s),
                (ab_hbm, ab_s),
                (q_hbm, q_s),
                (bucket_hbm, event_s.at[0]),
                (action_hbm, event_s.at[1]),
            )
        )
    ]
    mine = pl.ds(me * local, local)
    late = [
        pltpu.make_async_copy(source, target, late_sem.at[min(i, 1)])
        for i, (source, target) in enumerate(
            (
                (gain_hbm, gain_s),
                (nk_hbm.at[mine], mine_s.at[0]),
                (nv_hbm.at[mine], mine_s.at[1]),
                (gate_hbm.at[mine], mine_s.at[2]),
            )
        )
    ]
    for copy in early:
        copy.start()
    order = []
    acts = plan(seqs, local)
    groups = [act for act in acts if isinstance(act, list)]
    starts = [sum(len(group) for group in groups[:index]) for index in range(len(groups))]
    w_copy = pltpu.make_async_copy(w_hbm, w_s, late_sem.at[2])
    for index, group in enumerate(groups):
        if index == min(WHEN, len(groups) - 1):
            w_copy.start(priority=1)
        for turn, step in group:
            user = partner(me, step, seqs) * local + turn
            for part, source in enumerate((k_hbm, v_hbm)):
                pltpu.make_async_copy(
                    source.at[user], kv_s.at[len(order), part], kv_sem.at[index]
                ).start(priority=1)
            order.append((turn, step, user))
    for copy in late:
        copy.start()
    for copy in early[:4]:
        copy.wait()
    landed(event_s, in_sem.at[4])

    lane_of = lax.broadcasted_iota(jnp.int32, (users, cands, width), 2)
    query = q_s[...]
    for head in range(heads):
        qd_s[:, head * cands : (head + 1) * cands, :] = jnp.where(
            lane_of // size == head, query, jnp.zeros_like(query)
        )

    def table(ref, head):
        row = ref[head : head + 1, :] * LOG2E
        return jnp.concatenate([row, jnp.zeros((1, LANES - row.shape[1]), row.dtype)], axis=1)

    user_id = lax.broadcasted_iota(jnp.int32, (users, LANES), 0)
    limit = jnp.zeros((users, LANES), jnp.int32)
    for user in range(users):
        limit = jnp.where(user_id == user, len_ref[user], limit)
    limit = limit - me * block - lax.broadcasted_iota(jnp.int32, (users, LANES), 1)
    for head in range(heads):
        tb_row = jnp.broadcast_to(table(tb_s, head), (users, LANES))
        ab_row = jnp.broadcast_to(table(ab_s, head), (users, LANES))
        for chunk in range(block // LANES):
            lanes = slice(chunk * LANES, (chunk + 1) * LANES)
            bias = jnp.take_along_axis(tb_row, event_s[0, :, lanes], axis=1) + jnp.take_along_axis(
                ab_row, event_s[1, :, lanes], axis=1
            )
            bias_s[head, :, lanes] = jnp.where(limit > chunk * LANES, bias, INVALID)

    late[0].wait()
    landed(mine_s, late_sem.at[1])
    gate = mine_s[2].astype(jnp.float32)
    gated_s[...] = gain_s[...].reshape(1, 1, width) * (gate / (1.0 + jnp.exp(-gate)))

    def by_head(source):
        return jnp.concatenate(
            [source[:, head * size : (head + 1) * size] for head in range(heads)], axis=0
        )

    def score(slot):
        turn, step, user = order[slot]
        raw = lax.dot_general(qd_s[user], kv_s[slot, 0], NT, preferred_element_type=jnp.float32)
        bias = jnp.concatenate(
            [
                jnp.broadcast_to(bias_s[head, pl.ds(user, 1), :], (cands, block))
                for head in range(heads)
            ],
            axis=0,
        )
        scores = raw * scale + bias
        top = jnp.maximum(jnp.max(scores, axis=1, keepdims=True), FLOOR)
        fresh = None
        if step == 0:
            product = q_s[user].astype(jnp.float32) * mine_s[0, turn].astype(jnp.float32)
            own = jnp.sum(by_head(product), axis=1, keepdims=True) * scale
            top = jnp.maximum(top, own)
            fresh = jnp.exp2(own - top)
        weights = jnp.exp2(scores - top)
        total = jnp.sum(weights, axis=1, keepdims=True)
        if step == 0:
            total = total + fresh
            fresh = fresh * by_head(mine_s[1, turn].astype(jnp.float32))
        stats = column_to_row(top, 0, size) + column_to_row(total, rows, size)
        part_s[turn, step, rows : rows + 1, :] = stats
        return weights.astype(jnp.bfloat16), fresh

    def mix(slot, weights, fresh):
        turn, step, _ = order[slot]
        mixed = jnp.dot(weights, kv_s[slot, 1], preferred_element_type=jnp.float32)
        for head in range(heads):
            held = slice(head * cands, (head + 1) * cands)
            piece = mixed[held, head * size : (head + 1) * size]
            part_s[turn, step, held, :] = piece if fresh is None else piece + fresh[held]

    def exchange(turn, step):
        return pltpu.make_async_remote_copy(
            src_ref=part_s.at[turn, step],
            dst_ref=got_s.at[turn, step - 1],
            send_sem=send_sem,
            recv_sem=recv_sem.at[turn],
            device_id={"seq": partner(me, step, seqs)},
            device_id_type=MESH,
        )

    def receiver(rank):
        first = (slices - mh) // slices
        if rank == 0:
            return first * (slices - 1)
        below = slices - rank - 1
        return below + (below - mh - first * slices + 2 * slices) // (2 * slices)

    def spread(turn, rank):
        target = receiver(rank)
        return pltpu.make_async_remote_copy(
            src_ref=zpart_s.at[turn, target],
            dst_ref=zgot_s.at[turn, mh - (mh - target - 1 + slices) // slices],
            send_sem=zsend_sem,
            recv_sem=zrecv_sem.at[turn],
            device_id={"head": target},
            device_id_type=MESH,
        )

    later = []

    def combine(turn):
        landed(got_s.at[turn], recv_sem.at[turn])
        blocks = [part_s.at[turn, 0]] + [got_s.at[turn, step - 1] for step in range(1, seqs)]
        maxima = [row_to_column(ref[rows : rows + 1, :], 0, rows) for ref in blocks]
        sums = [row_to_column(ref[rows : rows + 1, :], rows, rows) for ref in blocks]
        top = functools.reduce(jnp.maximum, maxima)
        numer, denom = 0.0, 0.0
        for ref, high, amount in zip(blocks, maxima, sums):
            factor = jnp.exp2(high - top)
            numer = numer + factor * ref[:rows, :]
            denom = denom + factor * amount
        attended = numer / denom
        squares = jnp.sum(jnp.square(attended), axis=1, keepdims=True)
        square = squares[:cands]
        for head in range(1, heads):
            square = square + squares[head * cands : (head + 1) * cands]
        wide = jnp.concatenate(
            [attended[head * cands : (head + 1) * cands] for head in range(heads)], axis=1
        )
        hidden = (wide * gated_s[turn]).astype(jnp.bfloat16)
        projected = jnp.dot(hidden, w_s[...], preferred_element_type=jnp.float32)
        square_row = column_to_row(square, 0, LANES)
        for target in range(slices):
            for tile in range(tiles):
                first = target * out_cols + tile * LANES
                zpart_s[turn, target, tile * cands : (tile + 1) * cands, :] = projected[
                    :, first : first + LANES
                ]
            zpart_s[turn, target, tiles * cands : tiles * cands + 1, :] = square_row
        spread(turn, 0).start()
        later.append(turn)
        if turn == local - 1 or turn < local - DEFER:
            for held in later:
                for rank in range(1, slices - 1):
                    spread(held, rank).start()
            later.clear()

    def finish(turn):
        landed(zgot_s.at[turn], zrecv_sem.at[turn])
        total = zpart_s[turn, mh]
        for step in range(1, slices):
            total = total + zgot_s[turn, step - 1]
        column = row_to_column(total[tiles * cands :, :], 0, cands)
        factor = 1.0 / jnp.sqrt(column / (width * slices) + 1e-6)
        for tile in range(tiles):
            piece = total[tile * cands : (tile + 1) * cands] * factor
            out_ref[turn, :, tile * LANES : (tile + 1) * LANES] = piece.astype(out_ref.dtype)

    index = 0
    for act in acts:
        if isinstance(act, int):
            if act == 0:
                w_copy.wait()
            combine(act)
            continue
        first, last = starts[index], starts[index] + len(act)
        landed(kv_s.at[first:last], kv_sem.at[index])
        waiting = []
        for slot in range(first, last):
            waiting.append((slot, *score(slot)))
            if len(waiting) > 1:
                mix(*waiting.pop(0))
        mix(*waiting.pop(0))
        if index == 0:
            pl.semaphore_wait(barrier, seqs - 1 + slices - 1)
        for turn, step in act:
            if step:
                exchange(turn, step).start()
        index += 1
    for turn in range(local):
        finish(turn)
    landed(got_s, send_sem)
    landed(zgot_s, zsend_sem)


def body(
    query,
    new_key,
    new_value,
    keys,
    values,
    lengths,
    time_bucket,
    action,
    time_bias,
    action_bias,
    gate,
    norm_gain,
    w_out,
):
    users, block, width = keys.shape
    cands = query.shape[1]
    heads = time_bias.shape[1]
    size = width // heads
    seqs = lax.axis_size("seq")
    slices = lax.axis_size("head")
    local = users // seqs
    rows = heads * cands
    out_cols = w_out.shape[1] // slices
    tiles = out_cols // LANES
    groups = len([act for act in plan(seqs, local) if isinstance(act, list)])
    dims = (users, cands, block, heads, size, seqs, slices, local, out_cols)
    f32, bf16 = jnp.float32, jnp.bfloat16
    anywhere = pl.BlockSpec(memory_space=pltpu.HBM)
    return pl.pallas_call(
        functools.partial(kernel, dims),
        out_shape=jax.ShapeDtypeStruct((local, cands, out_cols), bf16),
        in_specs=[anywhere] * 13,
        out_specs=pl.BlockSpec(memory_space=pltpu.VMEM),
        scratch_shapes=[
            pltpu.SMEM((users,), jnp.int32),
            pltpu.VMEM((users, cands, width), bf16),
            pltpu.VMEM((3, local, cands, width), bf16),
            pltpu.VMEM((users, 2, block, width), bf16),
            pltpu.VMEM((2, users, block), jnp.int32),
            pltpu.VMEM(time_bias.T.shape, f32),
            pltpu.VMEM(action_bias.T.shape, f32),
            pltpu.VMEM((width,), f32),
            pltpu.VMEM(w_out.shape, bf16),
            pltpu.VMEM((users, rows, width), bf16),
            pltpu.VMEM((local, cands, width), f32),
            pltpu.VMEM((heads, users, block), f32),
            pltpu.VMEM((local, seqs, rows + 1, size), f32),
            pltpu.VMEM((local, seqs - 1, rows + 1, size), f32),
            pltpu.VMEM((local, slices, tiles * cands + 1, LANES), f32),
            pltpu.VMEM((local, slices - 1, tiles * cands + 1, LANES), f32),
            pltpu.SemaphoreType.DMA((groups,)),
            pltpu.SemaphoreType.DMA((5,)),
            pltpu.SemaphoreType.DMA((3,)),
            pltpu.SemaphoreType.DMA,
            pltpu.SemaphoreType.DMA((local,)),
            pltpu.SemaphoreType.DMA,
            pltpu.SemaphoreType.DMA((local,)),
        ],
        compiler_params=pltpu.CompilerParams(
            collective_id=0, has_side_effects=True, vmem_limit_bytes=52428800
        ),
    )(
        *(
            pltpu.with_memory_space_constraint(x, pltpu.HBM)
            for x in (
                lengths,
                query,
                new_key,
                new_value,
                keys,
                values,
                time_bucket,
                action,
                time_bias.T,
                action_bias.T,
                gate,
                norm_gain,
                w_out,
            )
        )
    )


def solution(mesh):
    placed = (
        P("groups", None, "head"),
        P("groups", None, "head"),
        P("groups", None, "head"),
        P("groups", "seq", "head"),
        P("groups", "seq", "head"),
        P("groups"),
        P("groups", "seq"),
        P("groups", "seq"),
        P(None, "head"),
        P(None, "head"),
        P("groups", None, "head"),
        P("head"),
        P("head", None),
    )
    return jax.shard_map(
        body,
        mesh=mesh,
        in_specs=placed,
        out_specs=P(("groups", "seq"), None, "head"),
        check_vma=False,
    )
```

```python
import functools
import math

import jax
import jax.numpy as jnp
from jax import lax
from jax.experimental import pallas as pl
from jax.experimental.pallas import tpu as pltpu
from jax.sharding import PartitionSpec as P

MESH = pl.DeviceIdType.MESH
LANES = 128
LOG2E = math.log2(math.e)
GROUP = 3
SIZES = [2, 3, 4, 2]
START = 11
DEFER = 2
WHEN = 4
INVALID = -1e30
FLOOR = -1e29
NT = (((1,), (1,)), ((), ()))


def partner(rank, step, count):
    result, bit = 0, 1
    while bit < count:
        held = (rank // bit) % 2
        result = result + bit * (1 - held if (step // bit) % 2 else held)
        bit *= 2
    return result


def plan(seqs, local):
    far = range(2, seqs)
    near = [step for step in (1, 0) if step < seqs]
    order = [(turn, step) for turn in range(min(local, 2)) for step in far]
    order += [(0, step) for step in near[:-1]]
    order += [(turn, step) for turn in range(2, local) for step in far]
    order += [(0, step) for step in near[-1:]]
    order += [(turn, step) for step in near for turn in range(1, local)]
    groups, first = [], 0
    for size in SIZES + [GROUP] * len(order):
        if first < len(order):
            groups.append(order[first : first + size])
            first += size
    acts, taken, ready, done = [], 0, [0] * local, 0
    for group in groups:
        acts.append(group)
        taken += len(group)
        for turn, _ in group:
            ready[turn] += 1
        if taken < len(order) and 16 * taken >= START * len(order) and ready[done] == seqs:
            acts.append(done)
            done += 1
    return acts + list(range(done, local))


def column_to_row(column, first, lanes):
    shape = (column.shape[0], lanes)
    row_id = lax.broadcasted_iota(jnp.int32, shape, 0)
    lane_id = lax.broadcasted_iota(jnp.int32, shape, 1)
    return jnp.sum(jnp.where(lane_id == row_id + first, column, 0.0), axis=0, keepdims=True)


def row_to_column(row, first, count):
    shape = (count, row.shape[1])
    row_id = lax.broadcasted_iota(jnp.int32, shape, 0)
    lane_id = lax.broadcasted_iota(jnp.int32, shape, 1)
    return jnp.sum(jnp.where(lane_id == row_id + first, row, 0.0), axis=1, keepdims=True)


def kernel(
    dims,
    len_hbm,
    q_hbm,
    nk_hbm,
    nv_hbm,
    k_hbm,
    v_hbm,
    bucket_hbm,
    action_hbm,
    tb_hbm,
    ab_hbm,
    gate_hbm,
    gain_hbm,
    w_hbm,
    out_ref,
    len_ref,
    q_s,
    mine_s,
    kv_s,
    event_s,
    tb_s,
    ab_s,
    gain_s,
    w_s,
    qd_s,
    gated_s,
    bias_s,
    part_s,
    got_s,
    zpart_s,
    zgot_s,
    kv_sem,
    in_sem,
    late_sem,
    send_sem,
    recv_sem,
    zsend_sem,
    zrecv_sem,
):
    users, cands, block, heads, size, seqs, slices, local, out_cols = dims
    rows = heads * cands
    width = heads * size
    tiles = out_cols // LANES
    me = lax.axis_index("seq")
    mh = lax.axis_index("head")

    def landed(ref, sem):
        pltpu.make_async_copy(ref, ref, sem).wait()

    scale = LOG2E / math.sqrt(size)

    barrier = pltpu.get_barrier_semaphore()
    for step in range(1, seqs):
        pl.semaphore_signal(
            barrier, inc=1, device_id={"seq": partner(me, step, seqs)}, device_id_type=MESH
        )
    for step in range(1, slices):
        pl.semaphore_signal(
            barrier, inc=1, device_id={"head": partner(mh, step, slices)}, device_id_type=MESH
        )

    early = [
        pltpu.make_async_copy(source, target, in_sem.at[min(i, 4)])
        for i, (source, target) in enumerate(
            (
                (len_hbm, len_ref),
                (tb_hbm, tb_s),
                (ab_hbm, ab_s),
                (q_hbm, q_s),
                (bucket_hbm, event_s.at[0]),
                (action_hbm, event_s.at[1]),
            )
        )
    ]
    mine = pl.ds(me * local, local)
    late = [
        pltpu.make_async_copy(source, target, late_sem.at[min(i, 1)])
        for i, (source, target) in enumerate(
            (
                (gain_hbm, gain_s),
                (nk_hbm.at[mine], mine_s.at[0]),
                (nv_hbm.at[mine], mine_s.at[1]),
                (gate_hbm.at[mine], mine_s.at[2]),
            )
        )
    ]
    for copy in early:
        copy.start()
    order = []
    acts = plan(seqs, local)
    groups = [act for act in acts if isinstance(act, list)]
    starts = [sum(len(group) for group in groups[:index]) for index in range(len(groups))]
    w_copy = pltpu.make_async_copy(w_hbm, w_s, late_sem.at[2])
    for index, group in enumerate(groups):
        if index == min(WHEN, len(groups) - 1):
            w_copy.start(priority=1)
        for turn, step in group:
            user = partner(me, step, seqs) * local + turn
            for part, source in enumerate((k_hbm, v_hbm)):
                pltpu.make_async_copy(
                    source.at[user], kv_s.at[len(order), part], kv_sem.at[index]
                ).start(priority=1)
            order.append((turn, step, user))
    for copy in late:
        copy.start()
    for copy in early[:4]:
        copy.wait()
    landed(event_s, in_sem.at[4])

    lane_of = lax.broadcasted_iota(jnp.int32, (users, cands, width), 2)
    query = q_s[...]
    for head in range(heads):
        qd_s[:, head * cands : (head + 1) * cands, :] = jnp.where(
            lane_of // size == head, query, jnp.zeros_like(query)
        )

    def table(ref, head):
        row = ref[head : head + 1, :] * LOG2E
        return jnp.concatenate([row, jnp.zeros((1, LANES - row.shape[1]), row.dtype)], axis=1)

    user_id = lax.broadcasted_iota(jnp.int32, (users, LANES), 0)
    limit = jnp.zeros((users, LANES), jnp.int32)
    for user in range(users):
        limit = jnp.where(user_id == user, len_ref[user], limit)
    limit = limit - me * block - lax.broadcasted_iota(jnp.int32, (users, LANES), 1)
    for head in range(heads):
        tb_row = jnp.broadcast_to(table(tb_s, head), (users, LANES))
        ab_row = jnp.broadcast_to(table(ab_s, head), (users, LANES))
        for chunk in range(block // LANES):
            lanes = slice(chunk * LANES, (chunk + 1) * LANES)
            bias = jnp.take_along_axis(tb_row, event_s[0, :, lanes], axis=1) + jnp.take_along_axis(
                ab_row, event_s[1, :, lanes], axis=1
            )
            bias_s[head, :, lanes] = jnp.where(limit > chunk * LANES, bias, INVALID)

    def by_head(source):
        return jnp.concatenate(
            [source[:, head * size : (head + 1) * size] for head in range(heads)], axis=0
        )

    def score(slot):
        turn, step, user = order[slot]
        raw = lax.dot_general(qd_s[user], kv_s[slot, 0], NT, preferred_element_type=jnp.float32)
        bias = jnp.concatenate(
            [
                jnp.broadcast_to(bias_s[head, pl.ds(user, 1), :], (cands, block))
                for head in range(heads)
            ],
            axis=0,
        )
        scores = raw * scale + bias
        top = jnp.maximum(jnp.max(scores, axis=1, keepdims=True), FLOOR)
        fresh = None
        if step == 0:
            product = q_s[user].astype(jnp.float32) * mine_s[0, turn].astype(jnp.float32)
            own = jnp.sum(by_head(product), axis=1, keepdims=True) * scale
            top = jnp.maximum(top, own)
            fresh = jnp.exp2(own - top)
        weights = jnp.exp2(scores - top)
        total = jnp.sum(weights, axis=1, keepdims=True)
        if step == 0:
            total = total + fresh
            fresh = fresh * by_head(mine_s[1, turn].astype(jnp.float32))
        stats = column_to_row(top, 0, size) + column_to_row(total, rows, size)
        part_s[turn, step, rows : rows + 1, :] = stats
        return weights.astype(jnp.bfloat16), fresh

    def mix(slot, weights, fresh):
        turn, step, _ = order[slot]
        mixed = jnp.dot(weights, kv_s[slot, 1], preferred_element_type=jnp.float32)
        for head in range(heads):
            held = slice(head * cands, (head + 1) * cands)
            piece = mixed[held, head * size : (head + 1) * size]
            part_s[turn, step, held, :] = piece if fresh is None else piece + fresh[held]

    def exchange(turn, step):
        return pltpu.make_async_remote_copy(
            src_ref=part_s.at[turn, step],
            dst_ref=got_s.at[turn, step - 1],
            send_sem=send_sem,
            recv_sem=recv_sem.at[turn],
            device_id={"seq": partner(me, step, seqs)},
            device_id_type=MESH,
        )

    def receiver(rank):
        first = (slices - mh) // slices
        if rank == 0:
            return first * (slices - 1)
        below = slices - rank - 1
        return below + (below - mh - first * slices + 2 * slices) // (2 * slices)

    def spread(turn, rank):
        target = receiver(rank)
        return pltpu.make_async_remote_copy(
            src_ref=zpart_s.at[turn, target],
            dst_ref=zgot_s.at[turn, mh - (mh - target - 1 + slices) // slices],
            send_sem=zsend_sem,
            recv_sem=zrecv_sem.at[turn],
            device_id={"head": target},
            device_id_type=MESH,
        )

    later = []

    def combine(turn):
        landed(got_s.at[turn], recv_sem.at[turn])
        blocks = [part_s.at[turn, 0]] + [got_s.at[turn, step - 1] for step in range(1, seqs)]
        maxima = [row_to_column(ref[rows : rows + 1, :], 0, rows) for ref in blocks]
        sums = [row_to_column(ref[rows : rows + 1, :], rows, rows) for ref in blocks]
        top = functools.reduce(jnp.maximum, maxima)
        numer, denom = 0.0, 0.0
        for ref, high, amount in zip(blocks, maxima, sums):
            factor = jnp.exp2(high - top)
            numer = numer + factor * ref[:rows, :]
            denom = denom + factor * amount
        attended = numer / denom
        squares = jnp.sum(jnp.square(attended), axis=1, keepdims=True)
        square = squares[:cands]
        for head in range(1, heads):
            square = square + squares[head * cands : (head + 1) * cands]
        wide = jnp.concatenate(
            [attended[head * cands : (head + 1) * cands] for head in range(heads)], axis=1
        )
        hidden = (wide * gated_s[turn]).astype(jnp.bfloat16)
        projected = jnp.dot(hidden, w_s[...], preferred_element_type=jnp.float32)
        square_row = column_to_row(square, 0, LANES)
        for target in range(slices):
            for tile in range(tiles):
                first = target * out_cols + tile * LANES
                zpart_s[turn, target, tile * cands : (tile + 1) * cands, :] = projected[
                    :, first : first + LANES
                ]
            zpart_s[turn, target, tiles * cands : tiles * cands + 1, :] = square_row
        spread(turn, 0).start()
        later.append(turn)
        if turn == local - 1 or turn < local - DEFER:
            for rank in range(1, slices - 1):
                for held in later:
                    spread(held, rank).start()
            later.clear()

    def finish(turn):
        landed(zgot_s.at[turn], zrecv_sem.at[turn])
        total = zpart_s[turn, mh]
        for step in range(1, slices):
            total = total + zgot_s[turn, step - 1]
        column = row_to_column(total[tiles * cands :, :], 0, cands)
        factor = 1.0 / jnp.sqrt(column / (width * slices) + 1e-6)
        for tile in range(tiles):
            piece = total[tile * cands : (tile + 1) * cands] * factor
            out_ref[turn, :, tile * LANES : (tile + 1) * LANES] = piece.astype(out_ref.dtype)

    index = 0
    for act in acts:
        if isinstance(act, int):
            if act == 0:
                w_copy.wait()
            combine(act)
            continue
        first, last = starts[index], starts[index] + len(act)
        landed(kv_s.at[first:last], kv_sem.at[index])
        waiting = []
        for slot in range(first, last):
            waiting.append((slot, *score(slot)))
            if len(waiting) > 1:
                mix(*waiting.pop(0))
        mix(*waiting.pop(0))
        if index == 0:
            pl.semaphore_wait(barrier, seqs - 1 + slices - 1)
        for turn, step in act:
            if step:
                exchange(turn, step).start()
        if index == 0:
            late[0].wait()
            landed(mine_s, late_sem.at[1])
            gate = mine_s[2].astype(jnp.float32)
            gated_s[...] = gain_s[...].reshape(1, 1, width) * (gate / (1.0 + jnp.exp(-gate)))
        index += 1
    for turn in range(local):
        finish(turn)
    landed(got_s, send_sem)
    landed(zgot_s, zsend_sem)


def body(
    query,
    new_key,
    new_value,
    keys,
    values,
    lengths,
    time_bucket,
    action,
    time_bias,
    action_bias,
    gate,
    norm_gain,
    w_out,
):
    users, block, width = keys.shape
    cands = query.shape[1]
    heads = time_bias.shape[1]
    size = width // heads
    seqs = lax.axis_size("seq")
    slices = lax.axis_size("head")
    local = users // seqs
    rows = heads * cands
    out_cols = w_out.shape[1] // slices
    tiles = out_cols // LANES
    groups = len([act for act in plan(seqs, local) if isinstance(act, list)])
    dims = (users, cands, block, heads, size, seqs, slices, local, out_cols)
    f32, bf16 = jnp.float32, jnp.bfloat16
    anywhere = pl.BlockSpec(memory_space=pltpu.HBM)
    return pl.pallas_call(
        functools.partial(kernel, dims),
        out_shape=jax.ShapeDtypeStruct((local, cands, out_cols), bf16),
        in_specs=[anywhere] * 13,
        out_specs=pl.BlockSpec(memory_space=pltpu.VMEM),
        scratch_shapes=[
            pltpu.SMEM((users,), jnp.int32),
            pltpu.VMEM((users, cands, width), bf16),
            pltpu.VMEM((3, local, cands, width), bf16),
            pltpu.VMEM((users, 2, block, width), bf16),
            pltpu.VMEM((2, users, block), jnp.int32),
            pltpu.VMEM(time_bias.T.shape, f32),
            pltpu.VMEM(action_bias.T.shape, f32),
            pltpu.VMEM((width,), f32),
            pltpu.VMEM(w_out.shape, bf16),
            pltpu.VMEM((users, rows, width), bf16),
            pltpu.VMEM((local, cands, width), f32),
            pltpu.VMEM((heads, users, block), f32),
            pltpu.VMEM((local, seqs, rows + 1, size), f32),
            pltpu.VMEM((local, seqs - 1, rows + 1, size), f32),
            pltpu.VMEM((local, slices, tiles * cands + 1, LANES), f32),
            pltpu.VMEM((local, slices - 1, tiles * cands + 1, LANES), f32),
            pltpu.SemaphoreType.DMA((groups,)),
            pltpu.SemaphoreType.DMA((5,)),
            pltpu.SemaphoreType.DMA((3,)),
            pltpu.SemaphoreType.DMA,
            pltpu.SemaphoreType.DMA((local,)),
            pltpu.SemaphoreType.DMA,
            pltpu.SemaphoreType.DMA((local,)),
        ],
        compiler_params=pltpu.CompilerParams(
            collective_id=0, has_side_effects=True, vmem_limit_bytes=52428800
        ),
    )(
        *(
            pltpu.with_memory_space_constraint(x, pltpu.HBM)
            for x in (
                lengths,
                query,
                new_key,
                new_value,
                keys,
                values,
                time_bucket,
                action,
                time_bias.T,
                action_bias.T,
                gate,
                norm_gain,
                w_out,
            )
        )
    )


def solution(mesh):
    placed = (
        P("groups", None, "head"),
        P("groups", None, "head"),
        P("groups", None, "head"),
        P("groups", "seq", "head"),
        P("groups", "seq", "head"),
        P("groups"),
        P("groups", "seq"),
        P("groups", "seq"),
        P(None, "head"),
        P(None, "head"),
        P("groups", None, "head"),
        P("head"),
        P("head", None),
    )
    return jax.shard_map(
        body,
        mesh=mesh,
        in_specs=placed,
        out_specs=P(("groups", "seq"), None, "head"),
        check_vma=False,
    )
```
